16 devices in a mesh: dp: 2 (over z), ep: 8 (over y, x, core).
Axes of the slice: x: 2, y: 2, z: 2, core: 2. Of those that a mesh axis runs over, the one named last changes fastest.
Arguments:
- x_tokens: bfloat16 [2048, 1024], P(('dp', 'ep'))
- expert_idx: int32 [2048, 8], P(('dp', 'ep'))
- d_out: bfloat16 [2048, 1024], P(('dp', 'ep'))
- norm_w: bfloat16 [1024], replicated
- w_router: bfloat16 [1024, 32], replicated
- b_router: float32 [32], replicated
- w_gate_up: bfloat16 [32, 1024, 1024], P('ep')
- b_gate_up: float32 [32, 1024], P('ep')
- w_down: bfloat16 [32, 512, 1024], P('ep')
- b_down: float32 [32, 1024], P('ep')
Outputs:
- output 1: bfloat16 [2048, 1024], P(('dp', 'ep'))
- output 2: bfloat16 [2048, 1024], P(('dp', 'ep'))
- output 3: float32 [32, 1024, 1024], P('ep')
- output 4: float32 [32, 1024], P('ep')
- output 5: float32 [32, 512, 1024], P('ep')
- output 6: float32 [32, 1024], P('ep')
- output 7: float32 [1024, 32], replicated
- output 8: float32 [32], replicated
- output 9: float32 [1024], replicated
All inputs are finite; a program needn't handle non-finite values.
Results may differ from the reference program's by a relative error of at most 0.00492042.
Values are sent between devices in bfloat16 or wider.
A program may use at most 1 GiB of HBM per device.

```python
import jax
import jax.numpy as jnp
from jax import lax

D_MODEL = 1024
D_FF = 512
EXPERTS = 32
TOP_K = 8
TOKENS = 2048
SWIGLU_LIMIT = 7.0
SIG_ALPHA = 1.702
NORM_EPS = 1e-5


def draw_routing(key_route, key_rank):
    noise = jax.random.randint(key_route, (TOKENS, EXPERTS), 0, 1000)
    expert_rank = jax.random.permutation(key_rank, EXPERTS)
    hot_bias = jnp.where(expert_rank < max(EXPERTS // 8, 1), 300, 0)
    scores = (noise + hot_bias[None, :]) * EXPERTS + jnp.arange(EXPERTS)[None, :]
    return lax.top_k(scores, TOP_K)[1].astype(jnp.int32)


def setup_inputs(seed: int = 0) -> dict:
    key_list = jax.random.split(jax.random.key(seed), 12)
    x_tokens = jax.random.normal(key_list[0], (TOKENS, D_MODEL), jnp.float32).astype(jnp.bfloat16)
    expert_idx = draw_routing(key_list[1], key_list[2])
    d_out = jax.random.normal(key_list[3], (TOKENS, D_MODEL), jnp.float32).astype(jnp.bfloat16)
    norm_w = (1.0 + 0.3 * jax.random.normal(key_list[4], (D_MODEL,), jnp.float32)).astype(jnp.bfloat16)
    w_router = (jax.random.normal(key_list[5], (D_MODEL, EXPERTS), jnp.float32) * D_MODEL ** -0.5).astype(jnp.bfloat16)
    b_router = 0.5 * jax.random.normal(key_list[6], (EXPERTS,), jnp.float32)
    w_gate_up = (jax.random.normal(key_list[7], (EXPERTS, D_MODEL, 2 * D_FF), jnp.float32) * (4.0 * D_MODEL ** -0.5)).astype(jnp.bfloat16)
    b_gate_up = 2.0 * jax.random.normal(key_list[8], (EXPERTS, 2 * D_FF), jnp.float32)
    w_down = (jax.random.normal(key_list[9], (EXPERTS, D_FF, D_MODEL), jnp.float32) * (0.1 * D_FF ** -0.5)).astype(jnp.bfloat16)
    b_down = 0.5 * jax.random.normal(key_list[10], (EXPERTS, D_MODEL), jnp.float32)
    return dict(x_tokens=x_tokens, expert_idx=expert_idx, d_out=d_out, norm_w=norm_w, w_router=w_router, b_router=b_router, w_gate_up=w_gate_up, b_gate_up=b_gate_up, w_down=w_down, b_down=b_down)


def reference(x_tokens, expert_idx, d_out, norm_w, w_router, b_router, w_gate_up, b_gate_up, w_down, b_down):
    x_float = x_tokens.astype(jnp.float32)
    inv_rms = lax.rsqrt(jnp.mean(x_float * x_float, axis=-1, keepdims=True) + NORM_EPS)
    normed = x_float * inv_rms
    h_bf = (normed * norm_w.astype(jnp.float32)).astype(jnp.bfloat16)
    logits = jnp.dot(h_bf, w_router, preferred_element_type=jnp.float32) + b_router
    route_prob = jax.nn.softmax(jnp.take_along_axis(logits, expert_idx, axis=1), axis=-1)
    dy_float = d_out.astype(jnp.float32)

    def expert_step(carry, expert_in):
        y_acc, dot_acc, dh_acc = carry
        w_gu, b_gu, w_dn, b_dn, expert_id = expert_in
        expert_hit = expert_idx == expert_id
        pair_coef = jnp.sum(jnp.where(expert_hit, route_prob, 0.0), axis=1)
        gate_up = jnp.dot(h_bf, w_gu, preferred_element_type=jnp.float32) + b_gu
        gate_pre = gate_up[:, :D_FF]
        up_pre = gate_up[:, D_FF:]
        gate_c = jnp.minimum(gate_pre, SWIGLU_LIMIT)
        up_c = jnp.clip(up_pre, -SWIGLU_LIMIT, SWIGLU_LIMIT)
        sig_gate = jax.nn.sigmoid(SIG_ALPHA * gate_c)
        act_bf = (gate_c * sig_gate * (up_c + 1.0)).astype(jnp.bfloat16)
        y_exp = jnp.dot(act_bf, w_dn, preferred_element_type=jnp.float32) + b_dn
        y_acc = y_acc + pair_coef[:, None] * y_exp
        dot_acc = dot_acc + jnp.where(expert_hit, jnp.sum(dy_float * y_exp, axis=1)[:, None], 0.0)
        v_pair = pair_coef[:, None] * dy_float
        v_bf = v_pair.astype(jnp.bfloat16)
        grad_dn = jnp.dot(act_bf.T, v_bf, preferred_element_type=jnp.float32)
        d_act = jnp.dot(v_bf, w_dn.T, preferred_element_type=jnp.float32)
        d_gate = jnp.where(gate_pre < SWIGLU_LIMIT, d_act * (up_c + 1.0) * sig_gate * (1.0 + SIG_ALPHA * gate_c * (1.0 - sig_gate)), 0.0)
        d_up = jnp.where((up_pre > -SWIGLU_LIMIT) & (up_pre < SWIGLU_LIMIT), d_act * gate_c * sig_gate, 0.0)
        d_gu = jnp.concatenate([d_gate, d_up], axis=1)
        d_gu_bf = d_gu.astype(jnp.bfloat16)
        grad_gu = jnp.dot(h_bf.T, d_gu_bf, preferred_element_type=jnp.float32)
        dh_acc = dh_acc + jnp.dot(d_gu_bf, w_gu.T, preferred_element_type=jnp.float32)
        return (y_acc, dot_acc, dh_acc), (grad_gu, jnp.sum(d_gu, axis=0), grad_dn, jnp.sum(v_pair, axis=0))

    carry_init = (jnp.zeros(x_float.shape, jnp.float32), jnp.zeros(route_prob.shape, jnp.float32), jnp.zeros(x_float.shape, jnp.float32))
    expert_ids = jnp.arange(EXPERTS, dtype=jnp.int32)
    carry_out, grads = lax.scan(expert_step, carry_init, (w_gate_up, b_gate_up, w_down, b_down, expert_ids))
    y_acc, dot_acc, dh_acc = carry_out
    grad_gate_up, grad_b_gate_up, grad_down, grad_b_down = grads
    y_out = (x_float + y_acc).astype(jnp.bfloat16)
    d_sel = route_prob * (dot_acc - jnp.sum(route_prob * dot_acc, axis=1, keepdims=True))
    expert_hits = expert_idx[:, :, None] == jnp.arange(EXPERTS)[None, None, :]
    d_logits = jnp.sum(jnp.where(expert_hits, d_sel[:, :, None], 0.0), axis=1)
    dlog_bf = d_logits.astype(jnp.bfloat16)
    grad_router = jnp.dot(h_bf.T, dlog_bf, preferred_element_type=jnp.float32)
    grad_b_router = jnp.sum(d_logits, axis=0)
    d_h = dh_acc + jnp.dot(dlog_bf, w_router.T, preferred_element_type=jnp.float32)
    grad_norm = jnp.sum(d_h * normed, axis=0)
    d_normed = d_h * norm_w.astype(jnp.float32)
    d_tokens = (dy_float + inv_rms * (d_normed - normed * jnp.mean(d_normed * normed, axis=-1, keepdims=True))).astype(jnp.bfloat16)
    return (y_out, d_tokens, grad_gate_up, grad_b_gate_up, grad_down, grad_b_down, grad_router, grad_b_router, grad_norm)
```

```python
import functools

import jax
import jax.numpy as jnp
from jax import lax
from jax.experimental import pallas as pl
from jax.experimental.pallas import tpu as pltpu
from jax.sharding import PartitionSpec as P

SWIGLU_LIMIT = 7.0
SIG_ALPHA = 1.702
NORM_EPS = 1e-5
F32 = jnp.float32
BF16 = jnp.bfloat16
MESH = pl.DeviceIdType.MESH
NT = (((1,), (1,)), ((), ()))
D = 1024
F = 512
E = 32
EL = 4
T = 128
WR = 2 * D + 128
ROWS = 32
COLS = 256


def block_kernel(x_ref, idx_ref, dout_ref, nw_ref, wr_ref, br_ref, wgu_hbm, bgu_ref, wdn_hbm, bdn_ref,
                 y_out, dt_out, gbgu_ref, gbdn_ref, g_out, h_hbm, a_hbm, c_hbm, v_hbm,
                 hd, pt, ph, pb, wgu, wdn, gu, da, a_st, c_st, v_st, yt, part, rd, rr, gath, accg, accd,
                 ag_s, ag_r, pt_s, pt_r, d2d_s, d2d_r, rs_s, rs_r, g_s, g_r, w_sem, st_sem, h_sem):
    d = lax.axis_index("dp")
    e = lax.axis_index("ep")
    k = e % 2
    cx = (e // 2) % 2
    cy = e // 4

    def chip(m):
        return ((cy + m // 2) % 2) * 2 + (cx + m % 2) % 2

    def ep_of(m, kk):
        return chip(m) * 2 + kk

    def dev(r):
        kk = (k + r % 2) % 2
        xx = (cx + (r // 2) % 2) % 2
        yy = (cy + (r // 4) % 2) % 2
        return ((d + r // 8) % 2, (yy * 2 + xx) * 2 + kk)

    sib = (d, e + 1 - 2 * k)
    zp = (1 - d, e)
    me = d * 8 + e

    for j in range(EL):
        pltpu.make_async_copy(wgu_hbm.at[j], wgu.at[j], w_sem.at[0, j]).start()
        pltpu.make_async_copy(wdn_hbm.at[j], wdn.at[j], w_sem.at[1, j]).start()

    barrier = pltpu.get_barrier_semaphore()

    @pl.loop(1, 16)
    def _(r):
        pl.semaphore_signal(barrier, inc=1, device_id=dev(r), device_id_type=MESH)

    x = x_ref[...].astype(F32)
    inv = lax.rsqrt(jnp.mean(x * x, axis=-1, keepdims=True) + NORM_EPS)
    normed = x * inv
    h = (normed * nw_ref[...].astype(F32)).astype(BF16)
    hd[me, :, :D] = h
    hd[me, :, D:] = dout_ref[...]
    logits = jnp.dot(h, wr_ref[...], preferred_element_type=F32) + br_ref[...]
    idx = idx_ref[...]
    lane = lax.broadcasted_iota(jnp.int32, (T, E), 1)
    hit = idx[:, 0:1] == lane
    for i in range(1, 8):
        hit = hit | (idx[:, i:i + 1] == lane)
    top = jnp.max(jnp.where(hit, logits, -jnp.inf), axis=-1, keepdims=True)
    ex = jnp.where(hit, jnp.exp(logits - top), 0.0)
    prob = ex / jnp.sum(ex, axis=-1, keepdims=True)
    ph[...] = prob
    pt[me] = prob.T

    pl.semaphore_wait(barrier, 15)

    def ag(i, g, to):
        return (pltpu.make_async_remote_copy(hd.at[g], hd.at[g], ag_s.at[i], ag_r.at[i], device_id=to, device_id_type=MESH),
                pltpu.make_async_remote_copy(pt.at[g], pt.at[g], pt_s.at[i], pt_r.at[i], device_id=to, device_id_type=MESH))

    def ag_send(i, g, to):
        for cp in ag(i, g, to):
            cp.start()

    def ag_wait(i, g):
        for cp in ag(i, g, sib):
            cp.wait_recv()

    ag_send(7, me, sib)
    ag_send(0, me, (d, ep_of(1, k)))
    ag_send(1, me, (d, ep_of(2, k)))
    ag_send(3, me, zp)
    ag_send(2, me, (d, ep_of(3, k)))

    accg[...] = jnp.zeros_like(accg)
    accd[...] = jnp.zeros_like(accd)

    def rd_copy(m):
        return pltpu.make_async_remote_copy(part.at[m, 1 - k], rd.at[m], d2d_s.at[m], d2d_r.at[m], device_id=sib, device_id_type=MESH)

    def rs_copy(m):
        return pltpu.make_async_remote_copy(part.at[m, k], rr.at[m - 1], rs_s.at[m - 1], rs_r.at[m - 1], device_id=(d, ep_of(m, k)), device_id_type=MESH)

    def st_copies(par, j, slot):
        return (pltpu.make_async_copy(a_st.at[par], a_hbm.at[j, pl.ds(slot * T, 2 * T)], st_sem.at[0, par]),
                pltpu.make_async_copy(c_st.at[par], c_hbm.at[j, pl.ds(slot * T, 2 * T)], st_sem.at[1, par]),
                pltpu.make_async_copy(v_st.at[par], v_hbm.at[j, pl.ds(slot * T, 2 * T)], st_sem.at[2, par]))

    def h_copy(slot):
        return pltpu.make_async_copy(hd.at[pl.ds(slot, 2), :, pl.ds(0, D)], h_hbm.at[pl.ds(slot, 2)], h_sem)

    def stage_probs(slot):
        sub = lax.broadcasted_iota(jnp.int32, (E, T), 0)
        for cc in range(2):
            rows = pt[slot + cc]
            for j in range(EL):
                row = jnp.sum(jnp.where(sub == 4 * e + j, rows, 0.0), axis=0, keepdims=True)
                pb[j, cc * T:(cc + 1) * T, :] = jnp.broadcast_to(row, (T, T)).T

    def expert(m, j, slot, own):
        par = j % 2
        hx = hd[pl.ds(slot, 2), :, :D].reshape(2 * T, D)
        gu[...] = jnp.dot(hx, wgu[j], preferred_element_type=F32)
        for r in range(0, 2 * T, ROWS):
            p = pb[j, r:r + ROWS, :]
            acc = None
            for c in range(0, D, COLS):
                dy = hd[slot + r // T, r % T:r % T + ROWS, D + c:D + c + COLS].astype(F32)
                v = jnp.concatenate([p] * (COLS // 128), axis=1) * dy
                v_st[par, r:r + ROWS, c:c + COLS] = v.astype(BF16)
                accd[j, :, c:c + COLS] += jnp.sum(v.reshape(ROWS // 8, 8, COLS), axis=0)
        da[...] = lax.dot_general(v_st[par], wdn[j], NT, preferred_element_type=F32)
        for r in range(0, 2 * T, ROWS):
            for c in range(0, F, COLS):
                gpre = gu[r:r + ROWS, c:c + COLS] + bgu_ref[j, :, c:c + COLS]
                upre = gu[r:r + ROWS, F + c:F + c + COLS] + bgu_ref[j, :, F + c:F + c + COLS]
                gc = jnp.minimum(gpre, SWIGLU_LIMIT)
                uc = jnp.clip(upre, -SWIGLU_LIMIT, SWIGLU_LIMIT)
                sg = jax.nn.sigmoid(SIG_ALPHA * gc)
                gs = gc * sg
                u1 = uc + 1.0
                a_st[par, r:r + ROWS, c:c + COLS] = (gs * u1).astype(BF16)
                dact = da[r:r + ROWS, c:c + COLS]
                dg = jnp.where(gpre < SWIGLU_LIMIT, dact * u1 * sg * (1.0 + SIG_ALPHA * gc * (1.0 - sg)), 0.0)
                du = jnp.where((upre > -SWIGLU_LIMIT) & (upre < SWIGLU_LIMIT), dact * gs, 0.0)
                c_st[par, r:r + ROWS, c:c + COLS] = dg.astype(BF16)
                c_st[par, r:r + ROWS, F + c:F + c + COLS] = du.astype(BF16)
                accg[j, :, c:c + COLS] += jnp.sum(dg.reshape(ROWS // 8, 8, COLS), axis=0)
                accg[j, :, F + c:F + c + COLS] += jnp.sum(du.reshape(ROWS // 8, 8, COLS), axis=0)
        if own:
            yt[...] = jnp.dot(a_st[par], wdn[j], preferred_element_type=F32)
            gu[...] = lax.dot_general(c_st[par], wgu[j], NT, preferred_element_type=F32)
            lanes = lax.broadcasted_iota(jnp.int32, (ROWS, 128), 1)
            for r in range(0, 2 * T, ROWS):
                p = pb[j, r:r + ROWS, :]
                cc, rt = r // T, r % T
                acc = jnp.zeros((ROWS, 128), F32)
                for c in range(0, D, 128):
                    yv = yt[r:r + ROWS, c:c + 128] + bdn_ref[j, :, c:c + 128]
                    dy = hd[slot + cc, rt:rt + ROWS, D + c:D + c + 128].astype(F32)
                    acc = acc + dy * yv
                    part[m, cc, rt:rt + ROWS, c:c + 128] += p * yv
                    part[m, cc, rt:rt + ROWS, D + c:D + c + 128] += gu[r:r + ROWS, c:c + 128]
                q = jnp.sum(acc, axis=1, keepdims=True)
                part[m, cc, rt:rt + ROWS, 2 * D:] += jnp.where(lanes == 4 * e + j, q, 0.0)

    def pre_expert(s, j, first):
        par = j % 2

        @pl.when(s * EL + j >= first)
        def _():
            for cp in st_copies(par, j, 0):
                cp.wait()

    @pl.loop(0, 4)
    def _(m):
        slot = d * 8 + chip(m) * 2
        ag_wait(7 + m, 0)
        h_copy(slot).start()
        stage_probs(slot)
        part[m] = jnp.zeros((2, T, WR), F32)

        @pl.loop(0, EL)
        def _(j):
            @pl.when(m == 0)
            def _():
                pltpu.make_async_copy(wgu_hbm.at[j], wgu.at[j], w_sem.at[0, j]).wait()
                pltpu.make_async_copy(wdn_hbm.at[j], wdn.at[j], w_sem.at[1, j]).wait()

            pre_expert(m, j, 2)
            expert(m, j, slot, True)
            for cp in st_copies(j % 2, j, slot):
                cp.start()

            @pl.when((j == 0) & (m >= 1))
            def _():
                rd_copy(m - 1).start()

            @pl.when((j == 1) & (m >= 1))
            def _():
                rd_copy(m - 1).wait_recv()
                part[m - 1, k] += rd[m - 1]

            @pl.when((j == 2) & (m >= 2))
            def _():
                rs_copy(m - 1).start()

            @pl.when((j == EL - 1) & (m < 3))
            def _():
                ag_wait(m, 0)
                g = d * 8 + ep_of(m + 1, k)
                ag_send(8 + m, g, sib)
                ag_send(4 + m, g, zp)

            @pl.when((j == EL - 1) & (m == 3))
            def _():
                ag_wait(3, 0)
                ag_send(11, (1 - d) * 8 + e, sib)

        h_copy(slot).wait()

    @pl.loop(0, 4)
    def _(m):
        slot = (1 - d) * 8 + chip(m) * 2
        ag_wait(11 + m, 0)
        h_copy(slot).start()
        stage_probs(slot)

        @pl.loop(0, EL)
        def _(j):
            pre_expert(m, j, 0)
            expert(m, j, slot, False)
            for cp in st_copies(j % 2, j, slot):
                cp.start()

            @pl.when((j == 0) & (m == 0))
            def _():
                rd_copy(3).start()

            @pl.when((j == 1) & (m == 0))
            def _():
                rd_copy(3).wait_recv()
                part[3, k] += rd[3]

            @pl.when((j == 2) & (m == 0))
            def _():
                rs_copy(3).start()

            @pl.when((j == EL - 1) & (m < 3))
            def _():
                ag_wait(4 + m, 0)
                ag_send(12 + m, (1 - d) * 8 + ep_of(m + 1, k), sib)

        h_copy(slot).wait()

    for par in range(2):
        for cp in st_copies(par, 0, 0):
            cp.wait()
    for j in range(EL):
        gbgu_ref[j] = jnp.sum(accg[j], axis=0, keepdims=True)
        gbdn_ref[j] = jnp.sum(accd[j], axis=0, keepdims=True)

    for m in range(1, 4):
        rs_copy(m).wait_recv()
    x = x_ref[...].astype(F32)
    inv = lax.rsqrt(jnp.mean(x * x, axis=-1, keepdims=True) + NORM_EPS)
    normed = x * inv
    tot = part[0, k] + rr[0] + rr[1] + rr[2]
    y_out[...] = (x + tot[:, :D]).astype(BF16)
    prob = ph[...]
    q = tot[:, 2 * D:2 * D + E]
    dlog = prob * (q - jnp.sum(prob * q, axis=1, keepdims=True))
    d_h = tot[:, D:2 * D] + lax.dot_general(dlog.astype(BF16), wr_ref[...], NT, preferred_element_type=F32)
    gath[me, :E, :] = dlog.T
    gn = jnp.sum(d_h * normed, axis=0, keepdims=True)
    for i in range(8):
        gath[me, E + i:E + i + 1, :] = gn[:, i * 128:(i + 1) * 128]
    dn = d_h * nw_ref[...].astype(F32)
    dt_out[...] = (dout_ref[...].astype(F32) + inv * (dn - normed * jnp.mean(dn * normed, axis=-1, keepdims=True))).astype(BF16)

    def g_copy(r):
        return pltpu.make_async_remote_copy(gath.at[me], gath.at[me], g_s.at[r], g_r.at[r], device_id=dev(r), device_id_type=MESH)

    @pl.loop(1, 16)
    def _(r):
        g_copy(r).start()

    for i in range(15):
        for cp in ag(i, 0, sib):
            cp.wait_send()
    for m in range(4):
        rd_copy(m).wait_send()
    for m in range(1, 4):
        rs_copy(m).wait_send()

    @pl.loop(1, 16)
    def _(r):
        g_copy(r).wait()

    g_out[...] = gath[...]


def grads_kernel(h_ref, a_ref, c_ref, v_ref, g_ref, ggu_ref, gdn_ref, gr_ref, gbr_ref, gn_ref, ht, at, dl):
    first = (pl.program_id(0) == 0) & (pl.program_id(1) == 0)

    @pl.when(first)
    def _():
        gbr = jnp.zeros((E, 128), F32)
        gn = jnp.zeros((8, 128), F32)
        for g in range(16):
            ht[:, g * T:(g + 1) * T] = h_ref[g].T
            dl[:, g * T:(g + 1) * T] = g_ref[g, :E, :].astype(BF16)
            gbr = gbr + g_ref[g, :E, :]
            gn = gn + g_ref[g, E:, :]
        gbr_ref[...] = jnp.sum(gbr, axis=1, keepdims=True)
        gn_ref[...] = gn
        gr_ref[...] = jnp.dot(dl[...], h_ref[...].reshape(16 * T, D), preferred_element_type=F32).T

    @pl.when(pl.program_id(1) == 0)
    def _():
        for g in range(16):
            at[:, g * T:(g + 1) * T] = a_ref[0, g * T:(g + 1) * T, :].T

    ggu_ref[0] = jnp.dot(ht[...], c_ref[0], preferred_element_type=F32)
    gdn_ref[0] = jnp.dot(at[...], v_ref[0], preferred_element_type=F32)


def block_body(x_tokens, expert_idx, d_out, norm_w, w_router, b_router, w_gate_up, b_gate_up, w_down, b_down):
    vm = pl.BlockSpec(memory_space=pltpu.VMEM)
    hb = pl.BlockSpec(memory_space=pl.ANY)
    s = jax.ShapeDtypeStruct
    n = 16 * T
    out = pl.pallas_call(
        block_kernel,
        out_shape=(s((T, D), BF16), s((T, D), BF16), s((EL, 1, D), F32), s((EL, 1, D), F32), s((16, 40, 128), F32),
                   s((16, T, D), BF16), s((EL, n, F), BF16), s((EL, n, 2 * F), BF16), s((EL, n, D), BF16)),
        in_specs=[vm, vm, vm, vm, vm, vm, hb, vm, hb, vm],
        out_specs=(vm, vm, vm, vm, vm, hb, hb, hb, hb),
        scratch_shapes=[
            pltpu.VMEM((16, T, 2 * D), BF16),
            pltpu.VMEM((16, E, T), F32),
            pltpu.VMEM((T, E), F32),
            pltpu.VMEM((EL, 2 * T, 128), F32),
            pltpu.VMEM((EL, D, 2 * F), BF16),
            pltpu.VMEM((EL, F, D), BF16),
            pltpu.VMEM((2 * T, 2 * F), F32),
            pltpu.VMEM((2 * T, F), F32),
            pltpu.VMEM((2, 2 * T, F), BF16),
            pltpu.VMEM((2, 2 * T, 2 * F), BF16),
            pltpu.VMEM((2, 2 * T, D), BF16),
            pltpu.VMEM((2 * T, D), F32),
            pltpu.VMEM((4, 2, T, WR), F32),
            pltpu.VMEM((4, T, WR), F32),
            pltpu.VMEM((3, T, WR), F32),
            pltpu.VMEM((16, 40, 128), F32),
            pltpu.VMEM((EL, 8, 2 * F), F32),
            pltpu.VMEM((EL, 8, D), F32),
            pltpu.SemaphoreType.DMA((15,)),
            pltpu.SemaphoreType.DMA((15,)),
            pltpu.SemaphoreType.DMA((15,)),
            pltpu.SemaphoreType.DMA((15,)),
            pltpu.SemaphoreType.DMA((4,)),
            pltpu.SemaphoreType.DMA((4,)),
            pltpu.SemaphoreType.DMA((3,)),
            pltpu.SemaphoreType.DMA((3,)),
            pltpu.SemaphoreType.DMA((16,)),
            pltpu.SemaphoreType.DMA((16,)),
            pltpu.SemaphoreType.DMA((2, EL)),
            pltpu.SemaphoreType.DMA((3, 2)),
            pltpu.SemaphoreType.DMA,
        ],
        compiler_params=pltpu.CompilerParams(collective_id=0, has_side_effects=True, vmem_limit_bytes=60 * 1024 * 1024),
        name="moe_block",
    )(x_tokens, expert_idx, d_out, norm_w.reshape(1, D), w_router, b_router.reshape(1, E),
      w_gate_up, b_gate_up.reshape(EL, 1, 2 * F), w_down, b_down.reshape(EL, 1, D))
    y_out, d_tok, gb_gu, gb_dn, gath, h_all, a_all, c_all, v_all = out
    half = D // 2
    g_gu, g_dn, g_r, g_br, g_n = pl.pallas_call(
        grads_kernel,
        grid=(EL, 2),
        out_shape=(s((EL, D, 2 * F), F32), s((EL, F, D), F32), s((D, E), F32), s((E, 1), F32), s((8, 128), F32)),
        in_specs=[
            pl.BlockSpec((16, T, D), lambda j, t: (0, 0, 0)),
            pl.BlockSpec((1, n, F), lambda j, t: (j, 0, 0)),
            pl.BlockSpec((1, n, half), lambda j, t: (j, 0, t)),
            pl.BlockSpec((1, n, half), lambda j, t: (j, 0, t)),
            pl.BlockSpec((16, 40, 128), lambda j, t: (0, 0, 0)),
        ],
        out_specs=(
            pl.BlockSpec((1, D, half), lambda j, t: (j, 0, t)),
            pl.BlockSpec((1, F, half), lambda j, t: (j, 0, t)),
            pl.BlockSpec((D, E), lambda j, t: (0, 0)),
            pl.BlockSpec((E, 1), lambda j, t: (0, 0)),
            pl.BlockSpec((8, 128), lambda j, t: (0, 0)),
        ),
        scratch_shapes=[pltpu.VMEM((D, n), BF16), pltpu.VMEM((F, n), BF16), pltpu.VMEM((E, n), BF16)],
        compiler_params=pltpu.CompilerParams(dimension_semantics=("arbitrary", "arbitrary"), vmem_limit_bytes=60 * 1024 * 1024),
        name="weight_grads",
    )(h_all, a_all, c_all, v_all, gath)
    return (y_out, d_tok, g_gu, gb_gu.reshape(EL, 2 * F), g_dn, gb_dn.reshape(EL, D), g_r, g_br.reshape(E), g_n.reshape(D))


def solution(mesh):
    tok = P(("dp", "ep"), None)
    w3 = P("ep", None, None)
    w2 = P("ep", None)
    in_specs = (tok, tok, tok, P(), P(), P(), w3, w2, w3, w2)
    out_specs = (tok, tok, w3, w2, w3, w2, P(), P(), P())
    return jax.shard_map(block_body, mesh=mesh, in_specs=in_specs, out_specs=out_specs, check_vma=False)
```

```python
import functools

import jax
import jax.numpy as jnp
from jax import lax
from jax.experimental import pallas as pl
from jax.experimental.pallas import tpu as pltpu
from jax.sharding import PartitionSpec as P

SWIGLU_LIMIT = 7.0
SIG_ALPHA = 1.702
NORM_EPS = 1e-5
F32 = jnp.float32
BF16 = jnp.bfloat16
MESH = pl.DeviceIdType.MESH
NT = (((1,), (1,)), ((), ()))
D = 1024
F = 512
E = 32
EL = 4
T = 128
WR = 2 * D + 128
CA = 1280
CB = WR - CA
MERGE_IT = 8
ROWS = 16
COLS = 128


def block_kernel(x_ref, idx_ref, dout_ref, nw_ref, wr_ref, br_ref, wgu_hbm, bgu_ref, wdn_hbm, bdn_ref,
                 y_out, dt_out, gbgu_ref, gbdn_ref, g_out, h_hbm, a_hbm, c_hbm, v_hbm,
                 hd, pt, ph, pb, wgu, wdn, gu, da, a_st, c_st, v_st, dyf, qs, bg, bd, part, rd, rxa, rxb, rya, ryb, ria, rib, gath, accg, accd,
                 ag_s, ag_r, pt_s, pt_r, d2d_s, d2d_r, rs_s, rs_r, g_s, g_r, w_sem, st_sem, h_sem):
    d = lax.axis_index("dp")
    e = lax.axis_index("ep")
    k = e % 2
    cx = (e // 2) % 2
    cy = e // 4

    def chip(m):
        return ((cy + m // 2) % 2) * 2 + (cx + m % 2) % 2

    def ep_of(m, kk):
        return chip(m) * 2 + kk

    def dev(r):
        kk = (k + r % 2) % 2
        xx = (cx + (r // 2) % 2) % 2
        yy = (cy + (r // 4) % 2) % 2
        return ((d + r // 8) % 2, (yy * 2 + xx) * 2 + kk)

    sib = (d, e + 1 - 2 * k)
    zp = (1 - d, e)
    me = d * 8 + e

    for j in range(EL):
        pltpu.make_async_copy(wgu_hbm.at[j], wgu.at[j], w_sem.at[0, j]).start()
        pltpu.make_async_copy(wdn_hbm.at[j], wdn.at[j], w_sem.at[1, j]).start()

    barrier = pltpu.get_barrier_semaphore()

    @pl.loop(1, 16)
    def _(r):
        pl.semaphore_signal(barrier, inc=1, device_id=dev(r), device_id_type=MESH)

    x = x_ref[...].astype(F32)
    inv = lax.rsqrt(jnp.mean(x * x, axis=-1, keepdims=True) + NORM_EPS)
    normed = x * inv
    h = (normed * nw_ref[...].astype(F32).reshape(1, D)).astype(BF16)
    hd[me, :, :D] = h
    hd[me, :, D:] = dout_ref[...]
    logits = lax.dot_general(h, wr_ref[...], NT, preferred_element_type=F32) + br_ref[...].reshape(1, E)
    idx = idx_ref[...].T
    lane = lax.broadcasted_iota(jnp.int32, (T, E), 1)
    hit = idx[:, 0:1] == lane
    for i in range(1, 8):
        hit = hit | (idx[:, i:i + 1] == lane)
    top = jnp.max(jnp.where(hit, logits, -jnp.inf), axis=-1, keepdims=True)
    ex = jnp.where(hit, jnp.exp(logits - top), 0.0)
    prob = ex / jnp.sum(ex, axis=-1, keepdims=True)
    ph[...] = prob
    pt[me] = prob.T

    pl.semaphore_wait(barrier, 15)

    def ag(i, g, to):
        return (pltpu.make_async_remote_copy(hd.at[g], hd.at[g], ag_s.at[i], ag_r.at[i], device_id=to, device_id_type=MESH),
                pltpu.make_async_remote_copy(pt.at[g], pt.at[g], pt_s.at[i], pt_r.at[i], device_id=to, device_id_type=MESH))

    def ag_send(i, g, to):
        for cp in ag(i, g, to):
            cp.start()

    def ag_wait(i, g):
        for cp in ag(i, g, sib):
            cp.wait_recv()

    ag_send(7, me, sib)
    ag_send(0, me, (d, ep_of(1, k)))
    ag_send(1, me, (d, ep_of(2, k)))
    ag_send(3, me, zp)
    ag_send(2, me, (d, ep_of(3, k)))

    for j in range(EL):
        bg[j] = bgu_ref[j:j + 1, :]
        bd[j] = bdn_ref[j:j + 1, :]
    accg[...] = jnp.zeros_like(accg)
    accd[...] = jnp.zeros_like(accd)

    def rd_copy(m):
        return pltpu.make_async_remote_copy(part.at[m, 1 - k], rd.at[m], d2d_s.at[m], d2d_r.at[m], device_id=sib, device_id_type=MESH)

    def rs_copy(i):
        m, first, dst, to = ((1, True, rxa, 1), (3, True, ria, 1), (1, False, rxb, 1),
                             (2, False, ryb, 2), (3, False, rib, 2), (2, True, rya, 2))[i]
        cols = pl.ds(0, CA) if first else pl.ds(CA, CB)
        return pltpu.make_async_remote_copy(part.at[m, k, :, cols], dst, rs_s.at[i], rs_r.at[i],
                                            device_id=(d, ep_of(to, k)), device_id_type=MESH)

    def merge(m, cols, src):
        part[m, k, :, cols] += src[...]

    def st_copies(par, j, slot):
        return (pltpu.make_async_copy(a_st.at[par], a_hbm.at[j, pl.ds(slot * T, 2 * T)], st_sem.at[0, par]),
                pltpu.make_async_copy(c_st.at[par], c_hbm.at[j, pl.ds(slot * T, 2 * T)], st_sem.at[1, par]),
                pltpu.make_async_copy(v_st.at[par], v_hbm.at[j, pl.ds(slot * T, 2 * T)], st_sem.at[2, par]))

    def h_copy(slot):
        return pltpu.make_async_copy(hd.at[pl.ds(slot, 2), :, pl.ds(0, D)], h_hbm.at[pl.ds(slot, 2)], h_sem)

    def stage_probs(slot):
        sub = lax.broadcasted_iota(jnp.int32, (E, T), 0)
        for cc in range(2):
            dyf[cc * T:(cc + 1) * T, :] = hd[slot + cc, :, D:].astype(F32)
            rows = pt[slot + cc]
            for j in range(EL):
                row = jnp.sum(jnp.where(sub == 4 * e + j, rows, 0.0), axis=0, keepdims=True)
                pb[j, cc * T:(cc + 1) * T, :] = jnp.broadcast_to(row, (T, T)).T

    def expert(m, j, slot, own):
        par = j % 2
        hx = hd[pl.ds(slot, 2), :, :D].reshape(2 * T, D)
        gu[...] = jnp.dot(hx, wgu[j], preferred_element_type=F32)
        for c in range(0, D, 128):
            acc = jnp.zeros((8, 128), F32)
            for r in range(0, 2 * T, ROWS):
                v = pb[j, r:r + ROWS, :] * dyf[r:r + ROWS, c:c + 128]
                v_st[par, r:r + ROWS, c:c + 128] = v.astype(BF16)
                acc = acc + jnp.sum(v.reshape(ROWS // 8, 8, 128), axis=0)
            accd[j, :, c:c + 128] += acc
        da[...] = lax.dot_general(v_st[par], wdn[j], NT, preferred_element_type=F32)
        for c in range(0, F, COLS):
            accl = jnp.zeros((8, COLS), F32)
            accu = jnp.zeros((8, COLS), F32)
            for r in range(0, 2 * T, ROWS):
                gpre = gu[r:r + ROWS, c:c + COLS] + bg[j, :, c:c + COLS]
                upre = gu[r:r + ROWS, F + c:F + c + COLS] + bg[j, :, F + c:F + c + COLS]
                gc = jnp.minimum(gpre, SWIGLU_LIMIT)
                uc = jnp.clip(upre, -SWIGLU_LIMIT, SWIGLU_LIMIT)
                sg = jax.nn.sigmoid(SIG_ALPHA * gc)
                gs = gc * sg
                u1 = uc + 1.0
                a_st[par, r:r + ROWS, c:c + COLS] = (gs * u1).astype(BF16)
                dact = da[r:r + ROWS, c:c + COLS]
                dg = jnp.where(gpre < SWIGLU_LIMIT, dact * u1 * sg * (1.0 + SIG_ALPHA * gc * (1.0 - sg)), 0.0)
                du = jnp.where(jnp.abs(upre) < SWIGLU_LIMIT, dact * gs, 0.0)
                c_st[par, r:r + ROWS, c:c + COLS] = dg.astype(BF16)
                c_st[par, r:r + ROWS, F + c:F + c + COLS] = du.astype(BF16)
                accl = accl + jnp.sum(dg.reshape(ROWS // 8, 8, COLS), axis=0)
                accu = accu + jnp.sum(du.reshape(ROWS // 8, 8, COLS), axis=0)
            accg[j, :, c:c + COLS] += accl
            accg[j, :, F + c:F + c + COLS] += accu
        if own:
            for c in range(0, D, 256):
                yv = jnp.dot(a_st[par], wdn[j, :, c:c + 256], preferred_element_type=F32)
                for r in range(0, 2 * T, ROWS):
                    p = pb[j, r:r + ROWS, :]
                    cc, rt = r // T, r % T
                    q = None
                    for b in range(0, 256, 128):
                        y1 = yv[r:r + ROWS, b:b + 128] + bd[j, :, c + b:c + b + 128]
                        part[m, cc, rt:rt + ROWS, c + b:c + b + 128] += p * y1
                        t = dyf[r:r + ROWS, c + b:c + b + 128] * y1
                        q = t if q is None else q + t
                    if c == 0:
                        qs[r:r + ROWS, :] = q
                    else:
                        qs[r:r + ROWS, :] += q
            for c in range(0, D, 256):
                dv = lax.dot_general(c_st[par], wgu[j, c:c + 256, :], NT, preferred_element_type=F32)
                part[m, :, :, D + c:D + c + 256] += dv.reshape(2, T, 256)
            lanes = lax.broadcasted_iota(jnp.int32, (T, 128), 1)
            for cc in range(2):
                q = jnp.sum(qs[cc * T:(cc + 1) * T, :], axis=1, keepdims=True)
                part[m, cc, :, 2 * D:] += jnp.where(lanes == 4 * e + j, q, 0.0)

    def pre_expert(s, j, first):
        par = j % 2

        @pl.when(s * EL + j >= first)
        def _():
            for cp in st_copies(par, j, 0):
                cp.wait()

    @pl.loop(0, 4)
    def _(s):
        m = s + (s // 2) * (1 - 2 * (s % 2))
        slot = d * 8 + chip(m) * 2
        ag_wait(7 + m, 0)
        h_copy(slot).start()
        stage_probs(slot)
        part[m] = jnp.zeros((2, T, WR), F32)

        @pl.loop(0, EL)
        def _(j):
            @pl.when(s == 0)
            def _():
                pltpu.make_async_copy(wgu_hbm.at[j], wgu.at[j], w_sem.at[0, j]).wait()
                pltpu.make_async_copy(wdn_hbm.at[j], wdn.at[j], w_sem.at[1, j]).wait()

            pre_expert(s, j, 2)
            expert(m, j, slot, True)
            it = s * EL + j

            @pl.when(it == 4)
            def _():
                rd_copy(0).wait_recv()
                merge(0, slice(None), rd.at[0])

            @pl.when(it == 8)
            def _():
                rd_copy(1).wait_recv()
                merge(1, slice(None), rd.at[1])

            @pl.when(it == 12)
            def _():
                rd_copy(3).wait_recv()
                merge(3, slice(None), rd.at[3])

            @pl.when(it == 15)
            def _():
                rs_copy(4).wait_recv()
                merge(1, slice(CA, WR), rib)

            for cp in st_copies(j % 2, j, slot):
                cp.start()

            def fetch(mm):
                ag_wait(mm - 1, 0)
                g = d * 8 + ep_of(mm, k)
                ag_send(7 + mm, g, sib)
                ag_send(3 + mm, g, zp)

            @pl.when(it == 3)
            def _():
                fetch(1)

            @pl.when(it == 5)
            def _():
                fetch(2)

            @pl.when(it == 6)
            def _():
                ag_wait(3, 0)
                ag_send(11, (1 - d) * 8 + e, sib)

            @pl.when(it == 7)
            def _():
                fetch(3)

            @pl.when(it == 8)
            def _():
                rs_copy(0).start()

            @pl.when(it == 12)
            def _():
                rs_copy(1).start()
                rs_copy(4).start()

            @pl.when(it == 15)
            def _():
                rs_copy(2).start()

            @pl.when(j == EL - 1)
            def _():
                rd_copy(m).start()

        h_copy(slot).wait()

    @pl.loop(0, 4)
    def _(m):
        slot = (1 - d) * 8 + chip(m) * 2
        ag_wait(11 + m, 0)
        h_copy(slot).start()
        stage_probs(slot)

        @pl.loop(0, EL)
        def _(j):
            pre_expert(m, j, 0)
            expert(m, j, slot, False)
            it = m * EL + j

            @pl.when(it == 1)
            def _():
                rd_copy(2).wait_recv()
                merge(2, slice(None), rd.at[2])

            @pl.when(it == MERGE_IT)
            def _():
                rs_copy(1).wait_recv()
                merge(2, slice(0, CA), ria)

            for cp in st_copies(j % 2, j, slot):
                cp.start()

            @pl.when((j == 2) & (m < 3))
            def _():
                ag_wait(4 + m, 0)
                ag_send(12 + m, (1 - d) * 8 + ep_of(m + 1, k), sib)

            @pl.when(it == 1)
            def _():
                rs_copy(3).start()

            @pl.when(it == MERGE_IT)
            def _():
                rs_copy(5).start()

        h_copy(slot).wait()

    for par in range(2):
        for cp in st_copies(par, 0, 0):
            cp.wait()
    for j in range(EL):
        gbgu_ref[j:j + 1, :] = jnp.sum(accg[j], axis=0, keepdims=True)
        gbdn_ref[j:j + 1, :] = jnp.sum(accd[j], axis=0, keepdims=True)

    for i in (0, 2, 3, 5):
        rs_copy(i).wait_recv()
    x = x_ref[...].astype(F32)
    inv = lax.rsqrt(jnp.mean(x * x, axis=-1, keepdims=True) + NORM_EPS)
    normed = x * inv
    tot_a = part[0, k, :, :CA] + rxa[...] + rya[...]
    tot_b = part[0, k, :, CA:] + rxb[...] + ryb[...]
    y_out[...] = (x + tot_a[:, :D]).astype(BF16)
    prob = ph[...]
    q = tot_b[:, 2 * D - CA:2 * D - CA + E]
    dlog = prob * (q - jnp.sum(prob * q, axis=1, keepdims=True))
    d_h = jnp.concatenate([tot_a[:, D:], tot_b[:, :2 * D - CA]], axis=1) + jnp.dot(dlog.astype(BF16), wr_ref[...], preferred_element_type=F32)
    gath[me, :E, :] = dlog.T
    gn = jnp.sum(d_h * normed, axis=0, keepdims=True)
    for i in range(8):
        gath[me, E + i:E + i + 1, :] = gn[:, i * 128:(i + 1) * 128]
    dn = d_h * nw_ref[...].astype(F32).reshape(1, D)
    dt_out[...] = (dout_ref[...].astype(F32) + inv * (dn - normed * jnp.mean(dn * normed, axis=-1, keepdims=True))).astype(BF16)

    def g_copy(r):
        return pltpu.make_async_remote_copy(gath.at[me], gath.at[me], g_s.at[r], g_r.at[r], device_id=dev(r), device_id_type=MESH)

    @pl.loop(1, 16)
    def _(r):
        g_copy(r).start()

    for i in range(15):
        for cp in ag(i, 0, sib):
            cp.wait_send()
    for m in range(4):
        rd_copy(m).wait_send()
    for i in range(6):
        rs_copy(i).wait_send()

    @pl.loop(1, 16)
    def _(r):
        g_copy(r).wait()

    g_out[...] = gath[...]


def grads_kernel(h_ref, a_ref, c_ref, v_ref, g_ref, yi_ref, ti_ref, bgi_ref, bdi_ref,
                 ggu_ref, gdn_ref, gr_ref, gbr_ref, gn_ref, yo_ref, to_ref, bgo_ref, bdo_ref, ht, at, dl):
    first = (pl.program_id(0) == 0) & (pl.program_id(1) == 0)

    @pl.when(first)
    def _():
        gbr = jnp.zeros((E, 128), F32)
        gn = jnp.zeros((8, 128), F32)
        for g in range(16):
            ht[:, g * T:(g + 1) * T] = h_ref[g].T
            dl[:, g * T:(g + 1) * T] = g_ref[g, :E, :].astype(BF16)
            gbr = gbr + g_ref[g, :E, :]
            gn = gn + g_ref[g, E:, :]
        gbr_ref[...] = jnp.sum(gbr.T, axis=0, keepdims=True)
        gn_ref[...] = gn
        yo_ref[...] = yi_ref[...]
        to_ref[...] = ti_ref[...]
        bgo_ref[...] = bgi_ref[...]
        bdo_ref[...] = bdi_ref[...]
        gr_ref[...] = jnp.dot(dl[...], h_ref[...].reshape(16 * T, D), preferred_element_type=F32)

    for g in range(16):
        at[:, g * T:(g + 1) * T] = a_ref[0, g * T:(g + 1) * T, :].T
    ggu_ref[0] = jnp.dot(ht[...], c_ref[0], preferred_element_type=F32)
    gdn_ref[0] = jnp.dot(at[...], v_ref[0], preferred_element_type=F32)


def block_body(x_tokens, expert_idx, d_out, norm_w, w_router, b_router, w_gate_up, b_gate_up, w_down, b_down):
    vm = pl.BlockSpec(memory_space=pltpu.VMEM)
    hb = pl.BlockSpec(memory_space=pl.ANY)
    s = jax.ShapeDtypeStruct
    n = 16 * T
    out = pl.pallas_call(
        block_kernel,
        out_shape=(s((T, D), BF16), s((T, D), BF16), s((EL, D), F32), s((EL, D), F32), s((16, 40, 128), F32),
                   s((16, T, D), BF16), s((EL, n, F), BF16), s((EL, n, 2 * F), BF16), s((EL, n, D), BF16)),
        in_specs=[vm, vm, vm, vm, vm, vm, hb, vm, hb, vm],
        out_specs=(vm, vm, vm, vm, vm, hb, hb, hb, hb),
        scratch_shapes=[
            pltpu.VMEM((16, T, 2 * D), BF16),
            pltpu.VMEM((16, E, T), F32),
            pltpu.VMEM((T, E), F32),
            pltpu.VMEM((EL, 2 * T, 128), F32),
            pltpu.VMEM((EL, D, 2 * F), BF16),
            pltpu.VMEM((EL, F, D), BF16),
            pltpu.VMEM((2 * T, 2 * F), F32),
            pltpu.VMEM((2 * T, F), F32),
            pltpu.VMEM((2, 2 * T, F), BF16),
            pltpu.VMEM((2, 2 * T, 2 * F), BF16),
            pltpu.VMEM((2, 2 * T, D), BF16),
            pltpu.VMEM((2 * T, D), F32),
            pltpu.VMEM((2 * T, 128), F32),
            pltpu.VMEM((EL, 1, 2 * F), F32),
            pltpu.VMEM((EL, 1, D), F32),
            pltpu.VMEM((4, 2, T, WR), F32),
            pltpu.VMEM((4, T, WR), F32),
            pltpu.VMEM((T, CA), F32),
            pltpu.VMEM((T, CB), F32),
            pltpu.VMEM((T, CA), F32),
            pltpu.VMEM((T, CB), F32),
            pltpu.VMEM((T, CA), F32),
            pltpu.VMEM((T, CB), F32),
            pltpu.VMEM((16, 40, 128), F32),
            pltpu.VMEM((EL, 8, 2 * F), F32),
            pltpu.VMEM((EL, 8, D), F32),
            pltpu.SemaphoreType.DMA((15,)),
            pltpu.SemaphoreType.DMA((15,)),
            pltpu.SemaphoreType.DMA((15,)),
            pltpu.SemaphoreType.DMA((15,)),
            pltpu.SemaphoreType.DMA((4,)),
            pltpu.SemaphoreType.DMA((4,)),
            pltpu.SemaphoreType.DMA((6,)),
            pltpu.SemaphoreType.DMA((6,)),
            pltpu.SemaphoreType.DMA((16,)),
            pltpu.SemaphoreType.DMA((16,)),
            pltpu.SemaphoreType.DMA((2, EL)),
            pltpu.SemaphoreType.DMA((3, 2)),
            pltpu.SemaphoreType.DMA,
        ],
        compiler_params=pltpu.CompilerParams(collective_id=0, has_side_effects=True, vmem_limit_bytes=60 * 1024 * 1024),
        name="moe_block",
    )(x_tokens, expert_idx.T, d_out, norm_w, w_router.T, b_router, w_gate_up, b_gate_up, w_down, b_down)
    y_out, d_tok, gb_gu, gb_dn, gath, h_all, a_all, c_all, v_all = out
    half = D // 2

    def full(shape):
        return pl.BlockSpec(shape, lambda j, t: (0, 0))

    g_gu, g_dn, g_r, g_br, g_n, y_out, d_tok, gb_gu, gb_dn = pl.pallas_call(
        grads_kernel,
        grid=(EL, 2),
        out_shape=(s((EL, D, 2 * F), F32), s((EL, F, D), F32), s((E, D), F32), s((1, E), F32), s((8, 128), F32),
                   s((T, D), BF16), s((T, D), BF16), s((EL, D), F32), s((EL, D), F32)),
        in_specs=[
            pl.BlockSpec((16, T, D), lambda j, t: (0, 0, 0)),
            pl.BlockSpec((1, n, F), lambda j, t: (j, 0, 0)),
            pl.BlockSpec((1, n, half), lambda j, t: (j, 0, t)),
            pl.BlockSpec((1, n, half), lambda j, t: (j, 0, t)),
            pl.BlockSpec((16, 40, 128), lambda j, t: (0, 0, 0)),
            full((T, D)), full((T, D)), full((EL, D)), full((EL, D)),
        ],
        out_specs=(
            pl.BlockSpec((1, D, half), lambda j, t: (j, 0, t)),
            pl.BlockSpec((1, F, half), lambda j, t: (j, 0, t)),
            pl.BlockSpec((E, D), lambda j, t: (0, 0)),
            pl.BlockSpec((1, E), lambda j, t: (0, 0)),
            pl.BlockSpec((8, 128), lambda j, t: (0, 0)),
            full((T, D)), full((T, D)), full((EL, D)), full((EL, D)),
        ),
        scratch_shapes=[pltpu.VMEM((D, n), BF16), pltpu.VMEM((F, n), BF16), pltpu.VMEM((E, n), BF16)],
        compiler_params=pltpu.CompilerParams(dimension_semantics=("arbitrary", "arbitrary"), vmem_limit_bytes=60 * 1024 * 1024),
        name="weight_grads",
    )(h_all, a_all, c_all, v_all, gath, y_out, d_tok, gb_gu, gb_dn)
    return (y_out, d_tok, g_gu, gb_gu, g_dn, gb_dn, g_r.T, g_br.reshape(E), g_n.reshape(D))


def solution(mesh):
    tok = P(("dp", "ep"), None)
    w3 = P("ep", None, None)
    w2 = P("ep", None)
    in_specs = (tok, tok, tok, P(), P(), P(), w3, w2, w3, w2)
    out_specs = (tok, tok, w3, w2, w3, w2, P(), P(), P())
    return jax.shard_map(block_body, mesh=mesh, in_specs=in_specs, out_specs=out_specs, check_vma=False)
```

```python
import functools

import jax
import jax.numpy as jnp
from jax import lax
from jax.experimental import pallas as pl
from jax.experimental.pallas import tpu as pltpu
from jax.sharding import PartitionSpec as P

SWIGLU_LIMIT = 7.0
SIG_ALPHA = 1.702
NORM_EPS = 1e-5
F32 = jnp.float32
BF16 = jnp.bfloat16
MESH = pl.DeviceIdType.MESH
NT = (((1,), (1,)), ((), ()))
D = 1024
F = 512
E = 32
EL = 4
T = 128
NC = 2
TT = NC * T
FF = NC * F
LN = 128
N = 16 * T
ROWS = 16
COLS = 128
MERGE_IT = 7
FETCH_D = 2


def mid_of(m):
    return (m + 1) // 2 % 2


def col_sum(v):
    return jnp.sum(v, axis=0, keepdims=True)


def row_mean(v):
    return jnp.mean(v, axis=-1, keepdims=True)


def slot_of(m, kk):
    mid = mid_of(m)
    return mid * (1 + m + 4 * kk) + (1 - mid) * (m // 3 * 4 + kk)


def place():
    d = lax.axis_index("dp")
    e = lax.axis_index("ep")
    return d, e, e % 2, (e // 2) % 2, e // 4


def block_kernel(x_ref, idx_ref, dout_ref, nw_ref, wr_ref, br_ref, wgu_hbm, bgu_ref, wdn_hbm, bdn_ref,
                 y_out, dt_out, gbgu_ref, gbdn_ref, gr_out, gn_out, ht_hbm, a_hbm, c_hbm, v_hbm,
                 hd, pt, pb, wgu, wdn, gu, da, a_st, c_st, v_st, dyf, qs, bg, bd, py, pd, rdy, rdd,
                 rxa, rxb, rya, ryb, ria, rib, qt, qbuf, dlog_s, gdl, ggn, ht, accg, accd,
                 ag_s, ag_r, pt_s, pt_r, d2d_s, d2d_r, rs_s, rs_r, q_s, q_r, dl_s, dl_r, gn_s, gn_r, w_sem, st_sem, h_sem):
    d, e, k, cx, cy = place()

    def ep_of(m, kk):
        return (((cy + m // 2) % 2) * 2 + (cx + m % 2) % 2) * 2 + kk

    def dev(r):
        return ((d + r // 8) % 2, ep_of((r // 2) % 4, (k + r % 2) % 2))

    sib = (d, e + 1 - 2 * k)
    zp = (1 - d, e)
    me = d * 8 + e

    for j in range(EL):
        pltpu.make_async_copy(wgu_hbm.at[j], wgu.at[j], w_sem.at[0, j]).start()
        pltpu.make_async_copy(wdn_hbm.at[j], wdn.at[j], w_sem.at[1, j]).start()

    barrier = pltpu.get_barrier_semaphore()

    @pl.loop(1, 16)
    def _(r):
        pl.semaphore_signal(barrier, inc=1, device_id=dev(r), device_id_type=MESH)

    nw = nw_ref[:].astype(F32).reshape(1, D)
    x = x_ref[:].astype(F32)
    inv = lax.rsqrt(row_mean(x * x) + NORM_EPS)
    h = (x * inv * nw).astype(BF16)
    hd[k, :, :D] = h
    hd[k, :, D:] = dout_ref[:]
    logits = lax.dot_general(h, wr_ref[:], NT, preferred_element_type=F32) + br_ref[:].reshape(1, E)
    idx = idx_ref[:].T
    lane = lax.broadcasted_iota(jnp.int32, (T, E), 1)
    hit = idx[:, 0:1] == lane
    for i in range(1, 8):
        hit = hit | (idx[:, i:i + 1] == lane)
    top = jnp.max(jnp.where(hit, logits, -jnp.inf), axis=-1, keepdims=True)
    ex = jnp.where(hit, jnp.exp(logits - top), 0.0)
    pt[k] = (ex / jnp.sum(ex, axis=-1, keepdims=True)).T

    pl.semaphore_wait(barrier, 15)

    def ag_copies(i, src, dst, to):
        return (pltpu.make_async_remote_copy(hd.at[src], hd.at[dst], ag_s.at[i], ag_r.at[i], device_id=to, device_id_type=MESH),
                pltpu.make_async_remote_copy(pt.at[src], pt.at[dst], pt_s.at[i], pt_r.at[i], device_id=to, device_id_type=MESH))

    def ag_send(i, src, dst, to):
        for cp in ag_copies(i, src, dst, to):
            cp.start()

    def ag_wait(i):
        for cp in ag_copies(i, 0, 0, sib):
            cp.wait_recv()

    def near(m):
        ag_send(m - 1, k, slot_of(m, k), (d, ep_of(m, k)))

    def fetch(m):
        ag_wait(m - 1)
        sl = slot_of(m, k)
        ag_send(7 + m, sl, sl, sib)
        ag_send(3 + m, sl, sl + 8, zp)

    def fetch_z(m):
        ag_wait(3 + m)
        sl = slot_of(m, k) + 8
        ag_send(11 + m, sl, sl, sib)

    ag_send(7, k, k, sib)

    @pl.when(k == 0)
    def _():
        near(1)
        near(2)

    ag_send(3, k, k + 8, zp)

    for j in range(EL):
        bg[j] = bgu_ref[j:j + 1, :]
        bd[j] = bdn_ref[j:j + 1, :]
    accg[:] = jnp.zeros_like(accg)
    accd[:] = jnp.zeros_like(accd)

    def mine(m):
        mid = mid_of(m)
        return mid * (1 + 2 * k) + (1 - mid) * (m // 3 * 2), mid * (m - 1) + (1 - mid) * k

    def theirs(m):
        mid = mid_of(m)
        return mid * (3 - 2 * k) + (1 - mid) * (m // 3 * 2), mid * (m - 1) + (1 - mid) * (1 - k)

    def d2d(m, hi):
        s, half = theirs(m)
        src, dst = (pd, rdd) if hi else (py, rdy)
        i = 2 * m + hi
        return pltpu.make_async_remote_copy(src.at[s, half], dst.at[m], d2d_s.at[i], d2d_r.at[i], device_id=sib, device_id_type=MESH)

    def pair_sum(m, hi):
        d2d(m, hi).wait_recv()
        s, half = mine(m)
        buf, src = (pd, rdd) if hi else (py, rdy)
        buf[s, half] += src[m]

    def rs_copy(i):
        m, hi, dst, to = ((1, 0, rxa, 1), (3, 0, ria, 1), (1, 1, rxb, 1),
                          (2, 1, ryb, 2), (3, 1, rib, 2), (2, 0, rya, 2))[i]
        s, half = mine(m)
        return pltpu.make_async_remote_copy((pd if hi else py).at[s, half], dst, rs_s.at[i], rs_r.at[i],
                                            device_id=(d, ep_of(to, k)), device_id_type=MESH)

    def q_copy(m, kk):
        i = m * 2 + (kk + k) % 2
        return pltpu.make_async_remote_copy(qt.at[slot_of(m, kk)], qbuf.at[e], q_s.at[i], q_r.at[i],
                                            device_id=(d, ep_of(m, kk)), device_id_type=MESH)

    def dl_copy(r):
        return pltpu.make_async_remote_copy(gdl.at[me], gdl.at[me], dl_s.at[r], dl_r.at[r], device_id=dev(r), device_id_type=MESH)

    def gn_copy(r):
        return pltpu.make_async_remote_copy(ggn.at[me], ggn.at[me], gn_s.at[r], gn_r.at[r], device_id=dev(r), device_id_type=MESH)

    def st_copies(par, j, slot):
        rows = pl.ds(slot * T, TT)
        return (pltpu.make_async_copy(a_st.at[par], a_hbm.at[j, rows], st_sem.at[0, par]),
                pltpu.make_async_copy(c_st.at[par], c_hbm.at[j, rows], st_sem.at[1, par]),
                pltpu.make_async_copy(v_st.at[par], v_hbm.at[j, rows], st_sem.at[2, par]))

    def ht_copy(i):
        cols = pl.ds(i * EL * T, EL * T)
        return pltpu.make_async_copy(ht.at[:, cols], ht_hbm.at[:, cols], h_sem.at[i])

    def stage_probs(slot):
        sub = lax.broadcasted_iota(jnp.int32, (E, T), 0)
        for cc in range(NC):
            dyf[cc * T:(cc + 1) * T, :] = hd[slot + cc, :, D:].astype(F32)
            rows = pt[slot + cc]
            for j in range(EL):
                row = col_sum(jnp.where(sub == 4 * e + j, rows, 0.0))
                pb[j, cc * T:(cc + 1) * T, :] = jnp.broadcast_to(row, (T, T)).T

    def expert(s, j, slot, own):
        par = j % 2
        hx = hd[pl.ds(slot, 2), :, :D].reshape(TT, D)
        gu[:] = jnp.dot(hx, wgu[j], preferred_element_type=F32)
        for c in range(0, D, LN):
            acc = jnp.zeros((8, LN), F32)
            for r in range(0, TT, ROWS):
                v = pb[j, r:r + ROWS, :] * dyf[r:r + ROWS, c:c + 128]
                v_st[par, r:r + ROWS, c:c + 128] = v.astype(BF16)
                acc = acc + jnp.sum(v.reshape(ROWS // 8, 8, LN), axis=0)
            accd[j, :, c:c + 128] += acc
        da[:] = lax.dot_general(v_st[par], wdn[j], NT, preferred_element_type=F32)
        for c in range(0, F, COLS):
            accl = jnp.zeros((8, COLS), F32)
            accu = jnp.zeros((8, COLS), F32)
            for r in range(0, TT, ROWS):
                gpre = gu[r:r + ROWS, c:c + COLS] + bg[j, :, c:c + COLS]
                upre = gu[r:r + ROWS, F + c:F + c + COLS] + bg[j, :, F + c:F + c + COLS]
                gc = jnp.minimum(gpre, SWIGLU_LIMIT)
                uc = jnp.clip(upre, -SWIGLU_LIMIT, SWIGLU_LIMIT)
                sg = jax.nn.sigmoid(SIG_ALPHA * gc)
                gs = gc * sg
                u1 = uc + 1.0
                a_st[par, r:r + ROWS, c:c + COLS] = (gs * u1).astype(BF16)
                dact = da[r:r + ROWS, c:c + COLS]
                dg = jnp.where(gpre < SWIGLU_LIMIT, dact * u1 * sg * (1.0 + SIG_ALPHA * gc * (1.0 - sg)), 0.0)
                du = jnp.where(jnp.abs(upre) < SWIGLU_LIMIT, dact * gs, 0.0)
                c_st[par, r:r + ROWS, c:c + COLS] = dg.astype(BF16)
                c_st[par, r:r + ROWS, F + c:F + c + COLS] = du.astype(BF16)
                accl = accl + jnp.sum(dg.reshape(ROWS // 8, 8, COLS), axis=0)
                accu = accu + jnp.sum(du.reshape(ROWS // 8, 8, COLS), axis=0)
            accg[j, :, c:c + COLS] += accl
            accg[j, :, F + c:F + c + COLS] += accu
        if own:
            for c in range(0, D, 256):
                yv = jnp.dot(a_st[par], wdn[j, :, c:c + 256], preferred_element_type=F32)
                for r in range(0, TT, ROWS):
                    p = pb[j, r:r + ROWS, :]
                    cc, rt = r // T, r % T
                    q = None
                    for b in range(0, 256, LN):
                        y1 = yv[r:r + ROWS, b:b + LN] + bd[j, :, c + b:c + b + LN]
                        py[s, cc, rt:rt + ROWS, c + b:c + b + LN] += p * y1
                        t = dyf[r:r + ROWS, c + b:c + b + LN] * y1
                        q = t if q is None else q + t
                    if c == 0:
                        qs[r:r + ROWS, :] = q
                    else:
                        qs[r:r + ROWS, :] += q
            for c in range(0, D, 256):
                dv = lax.dot_general(c_st[par], wgu[j, c:c + 256, :], NT, preferred_element_type=F32)
                pd[s, :, :, c:c + 256] += dv.reshape(2, T, 256)
            sub = lax.broadcasted_iota(jnp.int32, (8, T), 0)
            for cc in range(NC):
                row = col_sum(qs[cc * T:(cc + 1) * T, :].T)
                qt[slot + cc] = jnp.where(sub == j, row, qt[slot + cc])

    def drain(par):
        for cp in st_copies(par, 0, 0):
            cp.wait()

    @pl.loop(0, 4)
    def _(s):
        slot = 2 * s

        @pl.when(s == 0)
        def _():
            ag_wait(7)

        @pl.when(s == 2)
        def _():
            ag_wait(10)

        @pl.when(s + 2 * k == 3)
        def _():
            ag_wait(8)
            ag_wait(9)

        stage_probs(slot)
        py[s] = jnp.zeros((NC, T, D), F32)
        pd[s] = jnp.zeros((NC, T, D), F32)
        qt[slot] = jnp.zeros((8, T), F32)
        qt[slot + 1] = jnp.zeros((8, T), F32)

        @pl.loop(0, EL)
        def _(j):
            it = s * EL + j

            @pl.when(s == 0)
            def _():
                pltpu.make_async_copy(wgu_hbm.at[j], wgu.at[j], w_sem.at[0, j]).wait()
                pltpu.make_async_copy(wdn_hbm.at[j], wdn.at[j], w_sem.at[1, j]).wait()

            @pl.when(it >= 2)
            def _():
                drain(j % 2)

            expert(s, j, slot, True)

            @pl.when((it == 9) & (k == 0))
            def _():
                pair_sum(1, 1)
                pair_sum(2, 0)

            @pl.when(it == 6)
            def _():
                pair_sum(0, 0)
                pair_sum(0, 1)

            @pl.when(it == 12)
            def _():
                pair_sum(3, 0)
                pair_sum(3, 1)

            for cp in st_copies(j % 2, j, slot):
                cp.start()

            @pl.when((it == 1) & (k == 1))
            def _():
                near(1)
                near(2)

            @pl.when((it == 2) & (k == 0))
            def _():
                fetch(1)
                ag_send(2, slot_of(1, k), slot_of(3, k), (d, ep_of(2, k)))
                fetch(2)

            @pl.when((it == 5) & (k == 1))
            def _():
                fetch(2)
                ag_send(2, slot_of(2, k), slot_of(3, k), (d, ep_of(1, k)))
                fetch(1)

            @pl.when(it == 5)
            def _():
                fetch_z(0)

            @pl.when(it == 12 + 3 * k)
            def _():
                fetch_z(1)
                fetch_z(2)

            @pl.when(it == 12)
            def _():
                rs_copy(1).start()
                rs_copy(4).start()

            @pl.when(it == 3)
            def _():
                d2d(0, 0).start()
                d2d(0, 1).start()

            @pl.when(it == 15 - 8 * k)
            def _():
                d2d(1, 0).start()
                d2d(2, 1).start()
                d2d(1, 1).start()
                d2d(2, 0).start()

            @pl.when(it == 11)
            def _():
                d2d(3, 0).start()
                d2d(3, 1).start()

        @pl.when(s == 1)
        def _():
            ag_wait(11)
            stage_probs(8)

            @pl.loop(0, EL)
            def _(j):
                drain(j % 2)
                expert(0, j, 8, False)

                @pl.when((j == 1) & (k == 0))
                def _():
                    pair_sum(1, 0)
                    pair_sum(2, 1)

                for cp in st_copies(j % 2, j, 8):
                    cp.start()

                @pl.when((j == 1) & (k == 0))
                def _():
                    rs_copy(0).start()
                    rs_copy(3).start()

                @pl.when(j == FETCH_D)
                def _():
                    fetch(3)

        for half in range(NC):
            mid = s % 2
            m = mid * (1 + half) + (1 - mid) * (s // 2) * 3
            kk = mid * (s // 2) + (1 - mid) * half

            @pl.when((m > 0) | (kk != k))
            def _():
                q_copy(m, kk).start()

    @pl.loop(1, 4)
    def _(s):
        slot = 8 + 2 * s

        @pl.when(s == 2)
        def _():
            ag_wait(14)

        @pl.when(s + 2 * k == 3)
        def _():
            ag_wait(12)
            ag_wait(13)

        stage_probs(slot)

        @pl.loop(0, EL)
        def _(j):
            it = s * EL + j
            drain(j % 2)
            expert(s, j, slot, False)

            @pl.when((it == 5) & (k == 1))
            def _():
                pair_sum(1, 0)
                pair_sum(2, 1)

            @pl.when((it == 6) & (k == 1))
            def _():
                pair_sum(1, 1)
                pair_sum(2, 0)

            @pl.when(it == MERGE_IT)
            def _():
                rs_copy(1).wait_recv()
                s2, half2 = mine(2)
                py[s2, half2] += ria[:]
                rs_copy(4).wait_recv()
                s1, half1 = mine(1)
                pd[s1, half1] += rib[:]

            for cp in st_copies(j % 2, j, slot):
                cp.start()

            @pl.when((it == 5) & (k == 1))
            def _():
                rs_copy(0).start()
                rs_copy(3).start()

            @pl.when(it == MERGE_IT)
            def _():
                rs_copy(5).start()
                rs_copy(2).start()

            @pl.when(it == 6)
            def _():
                fetch_z(3)

            @pl.when(it == 8)
            def _():
                qbuf[e] = qt[k]
                for i in range(1, 8):
                    pltpu.make_async_remote_copy(qt.at[0], qbuf.at[e], q_s.at[i], q_r.at[i], device_id=sib, device_id_type=MESH).wait_recv()
                q = jnp.concatenate([qbuf[i, :EL, :] for i in range(8)], axis=0)
                prob = pt[k]
                dlog = prob * (q - col_sum(prob * q))
                dlog_s[:] = dlog
                gdl[me] = dlog.astype(BF16)

            @pl.when(it == 9)
            def _():
                @pl.loop(1, 16)
                def _(r):
                    dl_copy(r).start()

    for par in range(NC):
        drain(par)
    for j in range(EL):
        gbgu_ref[j:j + 1, :] = col_sum(accg[j])
        gbdn_ref[j:j + 1, :] = col_sum(accd[j])

    x = x_ref[:].astype(F32)
    inv = lax.rsqrt(row_mean(x * x) + NORM_EPS)
    normed = x * inv
    dlog = dlog_s[:].T
    dhr = jnp.dot(dlog.astype(BF16), wr_ref[:], preferred_element_type=F32)
    for i in (0, 3, 5, 2):
        rs_copy(i).wait_recv()
    d_h = pd[0, k] + rxb[:] + ryb[:] + dhr
    gn = col_sum(d_h * normed)
    for i in range(8):
        ggn[me, i:i + 1, :] = gn[:, i * 128:(i + 1) * 128]
    ggn[me, 8:16, :] = jnp.zeros((8, LN), F32)
    ggn[me, 8:9, :E] = col_sum(dlog)
    y_out[:] = (x + (py[0, k] + rxa[:] + rya[:])).astype(BF16)

    @pl.loop(1, 16)
    def _(r):
        gn_copy(r).start()

    dn = d_h * nw_ref[:].astype(F32).reshape(1, D)
    dt_out[:] = (dout_ref[:].astype(F32) + inv * (dn - normed * row_mean(dn * normed))).astype(BF16)

    for i in range(4):
        for g in range(EL * i, EL * i + EL):
            ht[:, g * T:(g + 1) * T] = hd[g, :, :D].T
        ht_copy(i).start()

    @pl.loop(1, 16)
    def _(r):
        dl_copy(r).wait()

    gr = jnp.zeros((E, D), F32)
    for g in range(16):
        dd, yy, xx, kk = g // 8, g // 4 % 2, g // 2 % 2, g % 2
        slot = 8 * ((dd + d) % 2) + slot_of((xx + cx) % 2 + 2 * ((yy + cy) % 2), kk)
        gr = gr + jnp.dot(gdl[g], hd[slot, :, :D], preferred_element_type=F32)
    gr_out[:] = gr

    for i in range(15):
        for cp in ag_copies(i, 0, 0, sib):
            cp.wait_send()
    for m in range(4):
        d2d(m, 0).wait_send()
        d2d(m, 1).wait_send()
    for i in range(6):
        rs_copy(i).wait_send()
    for i in range(1, 8):
        pltpu.make_async_remote_copy(qt.at[0], qbuf.at[e], q_s.at[i], q_r.at[i], device_id=sib, device_id_type=MESH).wait_send()

    @pl.loop(1, 16)
    def _(r):
        gn_copy(r).wait()

    gn_out[:] = ggn[:]
    for i in range(4):
        ht_copy(i).wait()


def grads_kernel(h_ref, a_ref, c_ref, v_ref, gri_ref, g_ref, yi_ref, ti_ref, bgi_ref, bdi_ref,
                 ggu_ref, gdn_ref, gr_ref, gbr_ref, gn_ref, yo_ref, to_ref, bgo_ref, bdo_ref, at):
    @pl.when((pl.program_id(0) == 0) & (pl.program_id(1) == 0))
    def _():
        gn = jnp.zeros((16, LN), F32)
        for g in range(16):
            gn = gn + g_ref[g]
        gr_ref[:] = gri_ref[:]
        gbr_ref[:] = gn[8:9, :E]
        gn_ref[:] = gn[:8]
        yo_ref[:] = yi_ref[:]
        to_ref[:] = ti_ref[:]
        bgo_ref[:] = bgi_ref[:]
        bdo_ref[:] = bdi_ref[:]

    for g in range(16):
        at[:, g * T:(g + 1) * T] = a_ref[0, g * T:(g + 1) * T, :].T
    ggu_ref[0] = jnp.dot(h_ref[:], c_ref[0], preferred_element_type=F32)
    gdn_ref[0] = jnp.dot(at[:], v_ref[0], preferred_element_type=F32)


def block_body(x_tokens, expert_idx, d_out, norm_w, w_router, b_router, w_gate_up, b_gate_up, w_down, b_down):
    vm = pl.BlockSpec(memory_space=pltpu.VMEM)
    hb = pl.BlockSpec(memory_space=pl.ANY)
    s = jax.ShapeDtypeStruct
    dma = pltpu.SemaphoreType.DMA
    out = pl.pallas_call(
        block_kernel,
        out_shape=(s((T, D), BF16), s((T, D), BF16), s((EL, D), F32), s((EL, D), F32), s((E, D), F32), s((16, 16, LN), F32),
                   s((D, N), BF16), s((EL, N, F), BF16), s((EL, N, FF), BF16), s((EL, N, D), BF16)),
        in_specs=[vm, vm, vm, vm, vm, vm, hb, vm, hb, vm],
        out_specs=(vm, vm, vm, vm, vm, vm, hb, hb, hb, hb),
        scratch_shapes=[
            pltpu.VMEM((16, T, 2 * D), BF16),
            pltpu.VMEM((16, E, T), F32),
            pltpu.VMEM((EL, TT, LN), F32),
            pltpu.VMEM((EL, D, FF), BF16),
            pltpu.VMEM((EL, F, D), BF16),
            pltpu.VMEM((TT, FF), F32),
            pltpu.VMEM((TT, F), F32),
            pltpu.VMEM((2, TT, F), BF16),
            pltpu.VMEM((2, TT, FF), BF16),
            pltpu.VMEM((2, TT, D), BF16),
            pltpu.VMEM((TT, D), F32),
            pltpu.VMEM((TT, LN), F32),
            pltpu.VMEM((EL, 1, FF), F32),
            pltpu.VMEM((EL, 1, D), F32),
            pltpu.VMEM((4, 2, T, D), F32),
            pltpu.VMEM((4, 2, T, D), F32),
            pltpu.VMEM((4, T, D), F32),
            pltpu.VMEM((4, T, D), F32),
        ] + [pltpu.VMEM((T, D), F32)] * 6 + [
            pltpu.VMEM((8, 8, T), F32),
            pltpu.VMEM((8, 8, T), F32),
            pltpu.VMEM((E, T), F32),
            pltpu.VMEM((16, E, T), BF16),
            pltpu.VMEM((16, 16, LN), F32),
            pltpu.VMEM((D, N), BF16),
            pltpu.VMEM((EL, 8, FF), F32),
            pltpu.VMEM((EL, 8, D), F32),
        ] + [dma((15,))] * 4 + [dma((8,))] * 2 + [dma((6,))] * 2 + [dma((8,))] * 2 + [dma((16,))] * 4 + [
            dma((2, EL)), dma((3, 2)), dma((4,)),
        ],
        compiler_params=pltpu.CompilerParams(collective_id=0, has_side_effects=True, vmem_limit_bytes=62 * 1024 * 1024),
        name="moe_block",
    )(x_tokens, expert_idx.T, d_out, norm_w, w_router.T, b_router, w_gate_up, b_gate_up, w_down, b_down)
    y_out, d_tok, gb_gu, gb_dn, g_r, gn_all, h_all, a_all, c_all, v_all = out
    half = D // 2

    def full(shape):
        return pl.BlockSpec(shape, lambda j, t: (0,) * len(shape))

    g_gu, g_dn, g_r, g_br, g_n, y_out, d_tok, gb_gu, gb_dn = pl.pallas_call(
        grads_kernel,
        grid=(EL, 2),
        out_shape=(s((EL, D, FF), F32), s((EL, F, D), F32), s((E, D), F32), s((1, E), F32), s((8, LN), F32),
                   s((T, D), BF16), s((T, D), BF16), s((EL, D), F32), s((EL, D), F32)),
        in_specs=[
            full((D, N)),
            pl.BlockSpec((1, N, F), lambda j, t: (j, 0, 0)),
            pl.BlockSpec((1, N, half), lambda j, t: (j, 0, t)),
            pl.BlockSpec((1, N, half), lambda j, t: (j, 0, t)),
            full((E, D)), full((16, 16, LN)), full((T, D)), full((T, D)), full((EL, D)), full((EL, D)),
        ],
        out_specs=(
            pl.BlockSpec((1, D, half), lambda j, t: (j, 0, t)),
            pl.BlockSpec((1, F, half), lambda j, t: (j, 0, t)),
            full((E, D)), full((1, E)), full((8, LN)), full((T, D)), full((T, D)), full((EL, D)), full((EL, D)),
        ),
        scratch_shapes=[pltpu.VMEM((F, N), BF16)],
        compiler_params=pltpu.CompilerParams(dimension_semantics=("arbitrary", "arbitrary"), vmem_limit_bytes=60 * 1024 * 1024),
        name="weight_grads",
    )(h_all, a_all, c_all, v_all, g_r, gn_all, y_out, d_tok, gb_gu, gb_dn)
    return (y_out, d_tok, g_gu, gb_gu, g_dn, gb_dn, g_r.T, g_br.reshape(E), g_n.reshape(D))


def solution(mesh):
    tok = P(("dp", "ep"), None)
    w3 = P("ep", None, None)
    w2 = P("ep", None)
    in_specs = (tok, tok, tok, P(), P(), P(), w3, w2, w3, w2)
    out_specs = (tok, tok, w3, w2, w3, w2, P(), P(), P())
    return jax.shard_map(block_body, mesh=mesh, in_specs=in_specs, out_specs=out_specs, check_vma=False)
```

```python
import functools

import jax
import jax.numpy as jnp
from jax import lax
from jax.experimental import pallas as pl
from jax.experimental.pallas import tpu as pltpu
from jax.sharding import PartitionSpec as P

SWIGLU_LIMIT = 7.0
SIG_ALPHA = 1.702
NORM_EPS = 1e-5
F32 = jnp.float32
BF16 = jnp.bfloat16
MESH = pl.DeviceIdType.MESH
NT = (((1,), (1,)), ((), ()))
D = 1024
F = 512
E = 32
EL = 4
T = 128
NC = 2
TT = NC * T
FF = NC * F
LN = 128
N = 16 * T
ROWS = 16
COLS = 128
MERGE_IT = 7
FETCH_D = 2


def mid_of(m):
    return (m + 1) // 2 % 2


def col_sum(v):
    return jnp.sum(v, axis=0, keepdims=True)


def row_mean(v):
    return jnp.mean(v, axis=-1, keepdims=True)


def slot_of(m, kk):
    mid = mid_of(m)
    return mid * (1 + m + 4 * kk) + (1 - mid) * (m // 3 * 4 + kk)


def place():
    d = lax.axis_index("dp")
    e = lax.axis_index("ep")
    return d, e, e % 2, (e // 2) % 2, e // 4


def block_kernel(x_ref, idx_ref, dout_ref, nw_ref, wr_ref, br_ref, wgu_hbm, bgu_ref, wdn_hbm, bdn_ref,
                 y_out, dt_out, gbgu_ref, gbdn_ref, gr_out, gn_out, ht_hbm, a_hbm, c_hbm, v_hbm,
                 hd, pt, pb, wgu, wdn, gu, da, a_st, c_st, v_st, dyf, qs, bg, bd, py, pd, rdy, rdd,
                 rxy, rxd, ryy, ryd, riy, rid, qt, qbuf, dlog_s, gdl, ggn, ht, accg, accd,
                 ag_s, ag_r, pt_s, pt_r, d2d_s, d2d_r, rs_s, rs_r, q_s, q_r, dl_s, dl_r, gn_s, gn_r, w_sem, st_sem, h_sem):
    d, e, k, cx, cy = place()

    def ep_of(m, kk):
        return (((cy + m // 2) % 2) * 2 + (cx + m % 2) % 2) * 2 + kk

    def dev(r):
        return ((d + r // 8) % 2, ep_of((r // 2) % 4, (k + r % 2) % 2))

    sib = (d, e + 1 - 2 * k)
    zp = (1 - d, e)
    me = d * 8 + e

    for j in range(EL):
        pltpu.make_async_copy(wgu_hbm.at[j], wgu.at[j], w_sem.at[0, j]).start()
        pltpu.make_async_copy(wdn_hbm.at[j], wdn.at[j], w_sem.at[1, j]).start()

    barrier = pltpu.get_barrier_semaphore()

    @pl.loop(1, 16)
    def _(r):
        pl.semaphore_signal(barrier, inc=1, device_id=dev(r), device_id_type=MESH)

    nw = nw_ref[:].astype(F32).reshape(1, D)
    x = x_ref[:].astype(F32)
    inv = lax.rsqrt(row_mean(x * x) + NORM_EPS)
    h = (x * inv * nw).astype(BF16)
    hd[k, :, :D] = h
    hd[k, :, D:] = dout_ref[:]
    logits = lax.dot_general(h, wr_ref[:], NT, preferred_element_type=F32) + br_ref[:].reshape(1, E)
    idx = idx_ref[:].T
    lane = lax.broadcasted_iota(jnp.int32, (T, E), 1)
    hit = idx[:, 0:1] == lane
    for i in range(1, 8):
        hit = hit | (idx[:, i:i + 1] == lane)
    top = jnp.max(jnp.where(hit, logits, -jnp.inf), axis=-1, keepdims=True)
    ex = jnp.where(hit, jnp.exp(logits - top), 0.0)
    pt[k] = (ex / jnp.sum(ex, axis=-1, keepdims=True)).T

    pl.semaphore_wait(barrier, 15)

    def ag_copies(i, src, dst, to):
        return (pltpu.make_async_remote_copy(hd.at[src], hd.at[dst], ag_s.at[i], ag_r.at[i], device_id=to, device_id_type=MESH),
                pltpu.make_async_remote_copy(pt.at[src], pt.at[dst], pt_s.at[i], pt_r.at[i], device_id=to, device_id_type=MESH))

    def ag_send(i, src, dst, to):
        for cp in ag_copies(i, src, dst, to):
            cp.start()

    def ag_wait(i):
        for cp in ag_copies(i, 0, 0, sib):
            cp.wait_recv()

    def near(m):
        ag_send(m - 1, k, slot_of(m, k), (d, ep_of(m, k)))

    def fetch(m):
        ag_wait(m - 1)
        sl = slot_of(m, k)
        ag_send(7 + m, sl, sl, sib)
        ag_send(3 + m, sl, sl + 8, zp)

    def fetch_z(m):
        ag_wait(3 + m)
        sl = slot_of(m, k) + 8
        ag_send(11 + m, sl, sl, sib)

    ag_send(7, k, k, sib)

    @pl.when(k == 0)
    def _():
        near(1)
        near(2)

    ag_send(3, k, k + 8, zp)

    for j in range(EL):
        bg[j] = bgu_ref[j:j + 1, :]
        bd[j] = bdn_ref[j:j + 1, :]
    accg[:] = jnp.zeros_like(accg)
    accd[:] = jnp.zeros_like(accd)

    def mine(m):
        mid = mid_of(m)
        return mid * (1 + 2 * k) + (1 - mid) * (m // 3 * 2), mid * (m - 1) + (1 - mid) * k

    def theirs(m):
        mid = mid_of(m)
        return mid * (3 - 2 * k) + (1 - mid) * (m // 3 * 2), mid * (m - 1) + (1 - mid) * (1 - k)

    def d2d(m, hi):
        s, half = theirs(m)
        src, dst = (pd, rdd) if hi else (py, rdy)
        i = 2 * m + hi
        return pltpu.make_async_remote_copy(src.at[s, half], dst.at[m], d2d_s.at[i], d2d_r.at[i], device_id=sib, device_id_type=MESH)

    def pair_sum(m, hi):
        d2d(m, hi).wait_recv()
        s, half = mine(m)
        buf, src = (pd, rdd) if hi else (py, rdy)
        buf[s, half] += src[m]

    def rs_copy(i, hi):
        m, first, dst, to = ((1, True, (rxy, rxd), 1), (3, True, (riy, rid), 1), (1, False, (rxy, rxd), 1),
                             (2, False, (ryy, ryd), 2), (3, False, (riy, rid), 2), (2, True, (ryy, ryd), 2))[i]
        s, half = mine(m)
        cols = pl.ds(0, F) if first else pl.ds(F, F)
        n = 6 * hi + i
        return pltpu.make_async_remote_copy((py, pd)[hi].at[s, half, :, cols], dst[hi].at[:, cols], rs_s.at[n], rs_r.at[n],
                                            device_id=(d, ep_of(to, k)), device_id_type=MESH)

    def rs_start(i, n):
        for hi in (1, 0):
            rs_copy(i, hi).start()
            rs_copy(n, hi).start()

    def pair_sums(m):
        pair_sum(m, 1)
        pair_sum(m, 0)

    def relay(hi):
        buf, src = ((py, riy), (pd, rid))[hi]
        rs_copy(1, hi).wait_recv()
        s2, half2 = mine(2)
        buf[s2, half2, :, :F] += src[:, :F]
        rs_copy(4, hi).wait_recv()
        s1, half1 = mine(1)
        buf[s1, half1, :, F:] += src[:, F:]

    def q_copy(m, kk):
        i = m * 2 + (kk + k) % 2
        return pltpu.make_async_remote_copy(qt.at[slot_of(m, kk)], qbuf.at[e], q_s.at[i], q_r.at[i],
                                            device_id=(d, ep_of(m, kk)), device_id_type=MESH)

    def dl_copy(r):
        return pltpu.make_async_remote_copy(gdl.at[me], gdl.at[me], dl_s.at[r], dl_r.at[r], device_id=dev(r), device_id_type=MESH)

    def gn_copy(r):
        return pltpu.make_async_remote_copy(ggn.at[me], ggn.at[me], gn_s.at[r], gn_r.at[r], device_id=dev(r), device_id_type=MESH)

    def st_copies(par, j, slot):
        rows = pl.ds(slot * T, TT)
        return (pltpu.make_async_copy(a_st.at[par], a_hbm.at[j, rows], st_sem.at[0, par]),
                pltpu.make_async_copy(c_st.at[par], c_hbm.at[j, rows], st_sem.at[1, par]),
                pltpu.make_async_copy(v_st.at[par], v_hbm.at[j, rows], st_sem.at[2, par]))

    def ht_copy(i):
        cols = pl.ds(i * EL * T, EL * T)
        return pltpu.make_async_copy(ht.at[:, cols], ht_hbm.at[:, cols], h_sem.at[i])

    def stage_probs(slot):
        sub = lax.broadcasted_iota(jnp.int32, (E, T), 0)
        for cc in range(NC):
            dyf[cc * T:(cc + 1) * T, :] = hd[slot + cc, :, D:].astype(F32)
            rows = pt[slot + cc]
            for j in range(EL):
                row = col_sum(jnp.where(sub == 4 * e + j, rows, 0.0))
                pb[j, cc * T:(cc + 1) * T, :] = jnp.broadcast_to(row, (T, T)).T

    def expert(s, j, slot, own):
        par = j % 2
        hx = hd[pl.ds(slot, 2), :, :D].reshape(TT, D)
        gu[:] = jnp.dot(hx, wgu[j], preferred_element_type=F32)
        for c in range(0, D, LN):
            acc = jnp.zeros((8, LN), F32)
            for r in range(0, TT, ROWS):
                v = pb[j, r:r + ROWS, :] * dyf[r:r + ROWS, c:c + 128]
                v_st[par, r:r + ROWS, c:c + 128] = v.astype(BF16)
                acc = acc + jnp.sum(v.reshape(ROWS // 8, 8, LN), axis=0)
            accd[j, :, c:c + 128] += acc
        da[:] = lax.dot_general(v_st[par], wdn[j], NT, preferred_element_type=F32)
        for c in range(0, F, COLS):
            accl = jnp.zeros((8, COLS), F32)
            accu = jnp.zeros((8, COLS), F32)
            for r in range(0, TT, ROWS):
                gpre = gu[r:r + ROWS, c:c + COLS] + bg[j, :, c:c + COLS]
                upre = gu[r:r + ROWS, F + c:F + c + COLS] + bg[j, :, F + c:F + c + COLS]
                gc = jnp.minimum(gpre, SWIGLU_LIMIT)
                sg = jax.nn.sigmoid(SIG_ALPHA * gc)
                gs = gc * sg
                u1 = jnp.clip(upre, -SWIGLU_LIMIT, SWIGLU_LIMIT) + 1.0
                a_st[par, r:r + ROWS, c:c + COLS] = (gs * u1).astype(BF16)
                gu[r:r + ROWS, c:c + COLS] = jnp.where(gpre < SWIGLU_LIMIT, u1 * (sg + SIG_ALPHA * gs * (1.0 - sg)), 0.0)
                gu[r:r + ROWS, F + c:F + c + COLS] = jnp.where(jnp.abs(upre) < SWIGLU_LIMIT, gs, 0.0)
            for r in range(0, TT, ROWS):
                dact = da[r:r + ROWS, c:c + COLS]
                dg = dact * gu[r:r + ROWS, c:c + COLS]
                du = dact * gu[r:r + ROWS, F + c:F + c + COLS]
                c_st[par, r:r + ROWS, c:c + COLS] = dg.astype(BF16)
                c_st[par, r:r + ROWS, F + c:F + c + COLS] = du.astype(BF16)
                accl = accl + jnp.sum(dg.reshape(ROWS // 8, 8, COLS), axis=0)
                accu = accu + jnp.sum(du.reshape(ROWS // 8, 8, COLS), axis=0)
            accg[j, :, c:c + COLS] += accl
            accg[j, :, F + c:F + c + COLS] += accu
        if own:
            for c in range(0, D, 256):
                yv = jnp.dot(a_st[par], wdn[j, :, c:c + 256], preferred_element_type=F32)
                for r in range(0, TT, ROWS):
                    p = pb[j, r:r + ROWS, :]
                    cc, rt = r // T, r % T
                    q = None
                    for b in range(0, 256, LN):
                        y1 = yv[r:r + ROWS, b:b + LN] + bd[j, :, c + b:c + b + LN]
                        py[s, cc, rt:rt + ROWS, c + b:c + b + LN] += p * y1
                        t = dyf[r:r + ROWS, c + b:c + b + LN] * y1
                        q = t if q is None else q + t
                    if c == 0:
                        qs[r:r + ROWS, :] = q
                    else:
                        qs[r:r + ROWS, :] += q
            for c in range(0, D, 256):
                dv = lax.dot_general(c_st[par], wgu[j, c:c + 256, :], NT, preferred_element_type=F32)
                pd[s, :, :, c:c + 256] += dv.reshape(2, T, 256)
            sub = lax.broadcasted_iota(jnp.int32, (8, T), 0)
            for cc in range(NC):
                row = col_sum(qs[cc * T:(cc + 1) * T, :].T)
                qt[slot + cc] = jnp.where(sub == j, row, qt[slot + cc])

    def drain(par):
        for cp in st_copies(par, 0, 0):
            cp.wait()

    @pl.loop(0, 4)
    def _(s):
        slot = 2 * s

        @pl.when(s == 0)
        def _():
            ag_wait(7)

        @pl.when(s == 2)
        def _():
            ag_wait(10)

        @pl.when(s + 2 * k == 3)
        def _():
            ag_wait(8)
            ag_wait(9)

        stage_probs(slot)
        py[s] = jnp.zeros((NC, T, D), F32)
        pd[s] = jnp.zeros((NC, T, D), F32)
        qt[slot] = jnp.zeros((8, T), F32)
        qt[slot + 1] = jnp.zeros((8, T), F32)

        @pl.loop(0, EL)
        def _(j):
            it = s * EL + j

            @pl.when(s == 0)
            def _():
                pltpu.make_async_copy(wgu_hbm.at[j], wgu.at[j], w_sem.at[0, j]).wait()
                pltpu.make_async_copy(wdn_hbm.at[j], wdn.at[j], w_sem.at[1, j]).wait()

            @pl.when(it >= 2)
            def _():
                drain(j % 2)

            expert(s, j, slot, True)

            @pl.when(it == 6)
            def _():
                pair_sum(0, 0)
                pair_sum(0, 1)

            @pl.when(it == 12)
            def _():
                pair_sums(3)

            for cp in st_copies(j % 2, j, slot):
                cp.start()

            @pl.when((it == 1) & (k == 1))
            def _():
                near(1)
                near(2)

            @pl.when((it == 2) & (k == 0))
            def _():
                fetch(1)
                ag_send(2, slot_of(1, k), slot_of(3, k), (d, ep_of(2, k)))
                fetch(2)

            @pl.when((it == 5) & (k == 1))
            def _():
                fetch(2)
                ag_send(2, slot_of(2, k), slot_of(3, k), (d, ep_of(1, k)))
                fetch(1)

            @pl.when(it == 5)
            def _():
                fetch_z(0)

            @pl.when(it == 12 + 3 * k)
            def _():
                fetch_z(1)
                fetch_z(2)

            @pl.when(it == 12)
            def _():
                rs_start(1, 4)

            @pl.when(it == 3)
            def _():
                d2d(0, 0).start()
                d2d(0, 1).start()

            @pl.when(it == 15 - 8 * k)
            def _():
                d2d(1, 0).start()
                d2d(2, 1).start()
                d2d(1, 1).start()
                d2d(2, 0).start()

            @pl.when(it == 11)
            def _():
                d2d(3, 0).start()
                d2d(3, 1).start()

        @pl.when(s == 1)
        def _():
            ag_wait(11)
            stage_probs(8)

            @pl.loop(0, EL)
            def _(j):
                drain(j % 2)
                expert(0, j, 8, False)

                @pl.when((j == 2) & (k == 0))
                def _():
                    pair_sums(1)
                    pair_sums(2)

                for cp in st_copies(j % 2, j, 8):
                    cp.start()

                @pl.when((j == 2) & (k == 0))
                def _():
                    rs_start(0, 3)

                @pl.when(j == FETCH_D)
                def _():
                    fetch(3)

        for half in range(NC):
            mid = s % 2
            m = mid * (1 + half) + (1 - mid) * (s // 2) * 3
            kk = mid * (s // 2) + (1 - mid) * half

            @pl.when((m > 0) | (kk != k))
            def _():
                q_copy(m, kk).start()

    @pl.loop(1, 4)
    def _(s):
        slot = 8 + 2 * s

        @pl.when(s == 2)
        def _():
            ag_wait(14)

        @pl.when(s + 2 * k == 3)
        def _():
            ag_wait(12)
            ag_wait(13)

        stage_probs(slot)

        @pl.loop(0, EL)
        def _(j):
            it = s * EL + j
            drain(j % 2)
            expert(s, j, slot, False)

            @pl.when((it == 6) & (k == 1))
            def _():
                pair_sums(1)
                pair_sums(2)

            @pl.when(it == MERGE_IT)
            def _():
                relay(1)

            @pl.when(it == MERGE_IT + 2)
            def _():
                relay(0)

            for cp in st_copies(j % 2, j, slot):
                cp.start()

            @pl.when((it == 6) & (k == 1))
            def _():
                rs_start(0, 3)

            @pl.when(it == MERGE_IT)
            def _():
                rs_copy(5, 1).start()
                rs_copy(2, 1).start()

            @pl.when(it == MERGE_IT + 2)
            def _():
                rs_copy(5, 0).start()
                rs_copy(2, 0).start()

            @pl.when(it == 6)
            def _():
                fetch_z(3)

            @pl.when(it == 8)
            def _():
                qbuf[e] = qt[k]
                for i in range(1, 8):
                    pltpu.make_async_remote_copy(qt.at[0], qbuf.at[e], q_s.at[i], q_r.at[i], device_id=sib, device_id_type=MESH).wait_recv()
                q = jnp.concatenate([qbuf[i, :EL, :] for i in range(8)], axis=0)
                prob = pt[k]
                dlog = prob * (q - col_sum(prob * q))
                dlog_s[:] = dlog
                gdl[me] = dlog.astype(BF16)

            @pl.when(it == 9)
            def _():
                @pl.loop(1, 16)
                def _(r):
                    dl_copy(r).start()

    for par in range(NC):
        drain(par)
    for j in range(EL):
        gbgu_ref[j:j + 1, :] = col_sum(accg[j])
        gbdn_ref[j:j + 1, :] = col_sum(accd[j])

    x = x_ref[:].astype(F32)
    inv = lax.rsqrt(row_mean(x * x) + NORM_EPS)
    normed = x * inv
    dlog = dlog_s[:].T
    dhr = jnp.dot(dlog.astype(BF16), wr_ref[:], preferred_element_type=F32)
    for i in (0, 3, 5, 2):
        rs_copy(i, 1).wait_recv()
    d_h = pd[0, k] + rxd[:] + ryd[:] + dhr
    gn = col_sum(d_h * normed)
    for i in range(8):
        ggn[me, i:i + 1, :] = gn[:, i * 128:(i + 1) * 128]
    ggn[me, 8:16, :] = jnp.zeros((8, LN), F32)
    ggn[me, 8:9, :E] = col_sum(dlog)

    @pl.loop(1, 16)
    def _(r):
        gn_copy(r).start()

    dn = d_h * nw_ref[:].astype(F32).reshape(1, D)
    dt_out[:] = (dout_ref[:].astype(F32) + inv * (dn - normed * row_mean(dn * normed))).astype(BF16)

    for i in range(4):
        for g in range(EL * i, EL * i + EL):
            ht[:, g * T:(g + 1) * T] = hd[g, :, :D].T
        ht_copy(i).start()

    @pl.loop(1, 16)
    def _(r):
        dl_copy(r).wait()

    gr = jnp.zeros((E, D), F32)
    for g in range(16):
        dd, yy, xx, kk = g // 8, g // 4 % 2, g // 2 % 2, g % 2
        slot = 8 * ((dd + d) % 2) + slot_of((xx + cx) % 2 + 2 * ((yy + cy) % 2), kk)
        gr = gr + jnp.dot(gdl[g], hd[slot, :, :D], preferred_element_type=F32)
    gr_out[:] = gr
    for i in (0, 3, 5, 2):
        rs_copy(i, 0).wait_recv()
    y_out[:] = (x_ref[:].astype(F32) + (py[0, k] + rxy[:] + ryy[:])).astype(BF16)

    for i in range(15):
        for cp in ag_copies(i, 0, 0, sib):
            cp.wait_send()
    for m in range(4):
        d2d(m, 0).wait_send()
        d2d(m, 1).wait_send()
    for i in range(6):
        rs_copy(i, 0).wait_send()
        rs_copy(i, 1).wait_send()
    for i in range(1, 8):
        pltpu.make_async_remote_copy(qt.at[0], qbuf.at[e], q_s.at[i], q_r.at[i], device_id=sib, device_id_type=MESH).wait_send()

    @pl.loop(1, 16)
    def _(r):
        gn_copy(r).wait()

    gn_out[:] = ggn[:]
    for i in range(4):
        ht_copy(i).wait()


def grads_kernel(h_ref, a_ref, c_ref, v_ref, gri_ref, g_ref, yi_ref, ti_ref, bgi_ref, bdi_ref,
                 ggu_ref, gdn_ref, gr_ref, gbr_ref, gn_ref, yo_ref, to_ref, bgo_ref, bdo_ref, at):
    @pl.when((pl.program_id(0) == 0) & (pl.program_id(1) == 0))
    def _():
        gn = jnp.zeros((16, LN), F32)
        for g in range(16):
            gn = gn + g_ref[g]
        gr_ref[:] = gri_ref[:]
        gbr_ref[:] = gn[8:9, :E]
        gn_ref[:] = gn[:8]
        yo_ref[:] = yi_ref[:]
        to_ref[:] = ti_ref[:]
        bgo_ref[:] = bgi_ref[:]
        bdo_ref[:] = bdi_ref[:]

    for g in range(16):
        at[:, g * T:(g + 1) * T] = a_ref[0, g * T:(g + 1) * T, :].T
    ggu_ref[0] = jnp.dot(h_ref[:], c_ref[0], preferred_element_type=F32)
    gdn_ref[0] = jnp.dot(at[:], v_ref[0], preferred_element_type=F32)


def block_body(x_tokens, expert_idx, d_out, norm_w, w_router, b_router, w_gate_up, b_gate_up, w_down, b_down):
    vm = pl.BlockSpec(memory_space=pltpu.VMEM)
    hb = pl.BlockSpec(memory_space=pl.ANY)
    s = jax.ShapeDtypeStruct
    dma = pltpu.SemaphoreType.DMA
    out = pl.pallas_call(
        block_kernel,
        out_shape=(s((T, D), BF16), s((T, D), BF16), s((EL, D), F32), s((EL, D), F32), s((E, D), F32), s((16, 16, LN), F32),
                   s((D, N), BF16), s((EL, N, F), BF16), s((EL, N, FF), BF16), s((EL, N, D), BF16)),
        in_specs=[vm, vm, vm, vm, vm, vm, hb, vm, hb, vm],
        out_specs=(vm, vm, vm, vm, vm, vm, hb, hb, hb, hb),
        scratch_shapes=[
            pltpu.VMEM((16, T, 2 * D), BF16),
            pltpu.VMEM((16, E, T), F32),
            pltpu.VMEM((EL, TT, LN), F32),
            pltpu.VMEM((EL, D, FF), BF16),
            pltpu.VMEM((EL, F, D), BF16),
            pltpu.VMEM((TT, FF), F32),
            pltpu.VMEM((TT, F), F32),
            pltpu.VMEM((2, TT, F), BF16),
            pltpu.VMEM((2, TT, FF), BF16),
            pltpu.VMEM((2, TT, D), BF16),
            pltpu.VMEM((TT, D), F32),
            pltpu.VMEM((TT, LN), F32),
            pltpu.VMEM((EL, 1, FF), F32),
            pltpu.VMEM((EL, 1, D), F32),
            pltpu.VMEM((4, 2, T, D), F32),
            pltpu.VMEM((4, 2, T, D), F32),
            pltpu.VMEM((4, T, D), F32),
            pltpu.VMEM((4, T, D), F32),
        ] + [pltpu.VMEM((T, D), F32)] * 6 + [
            pltpu.VMEM((8, 8, T), F32),
            pltpu.VMEM((8, 8, T), F32),
            pltpu.VMEM((E, T), F32),
            pltpu.VMEM((16, E, T), BF16),
            pltpu.VMEM((16, 16, LN), F32),
            pltpu.VMEM((D, N), BF16),
            pltpu.VMEM((EL, 8, FF), F32),
            pltpu.VMEM((EL, 8, D), F32),
        ] + [dma((15,))] * 4 + [dma((8,))] * 2 + [dma((12,))] * 2 + [dma((8,))] * 2 + [dma((16,))] * 4 + [
            dma((2, EL)), dma((3, 2)), dma((4,)),
        ],
        compiler_params=pltpu.CompilerParams(collective_id=0, has_side_effects=True, vmem_limit_bytes=62 * 1024 * 1024),
        name="moe_block",
    )(x_tokens, expert_idx.T, d_out, norm_w, w_router.T, b_router, w_gate_up, b_gate_up, w_down, b_down)
    y_out, d_tok, gb_gu, gb_dn, g_r, gn_all, h_all, a_all, c_all, v_all = out
    half = D // 2

    def full(shape):
        return pl.BlockSpec(shape, lambda j, t: (0,) * len(shape))

    g_gu, g_dn, g_r, g_br, g_n, y_out, d_tok, gb_gu, gb_dn = pl.pallas_call(
        grads_kernel,
        grid=(EL, 2),
        out_shape=(s((EL, D, FF), F32), s((EL, F, D), F32), s((E, D), F32), s((1, E), F32), s((8, LN), F32),
                   s((T, D), BF16), s((T, D), BF16), s((EL, D), F32), s((EL, D), F32)),
        in_specs=[
            full((D, N)),
            pl.BlockSpec((1, N, F), lambda j, t: (j, 0, 0)),
            pl.BlockSpec((1, N, half), lambda j, t: (j, 0, t)),
            pl.BlockSpec((1, N, half), lambda j, t: (j, 0, t)),
            full((E, D)), full((16, 16, LN)), full((T, D)), full((T, D)), full((EL, D)), full((EL, D)),
        ],
        out_specs=(
            pl.BlockSpec((1, D, half), lambda j, t: (j, 0, t)),
            pl.BlockSpec((1, F, half), lambda j, t: (j, 0, t)),
            full((E, D)), full((1, E)), full((8, LN)), full((T, D)), full((T, D)), full((EL, D)), full((EL, D)),
        ),
        scratch_shapes=[pltpu.VMEM((F, N), BF16)],
        compiler_params=pltpu.CompilerParams(dimension_semantics=("arbitrary", "arbitrary"), vmem_limit_bytes=60 * 1024 * 1024),
        name="weight_grads",
    )(h_all, a_all, c_all, v_all, g_r, gn_all, y_out, d_tok, gb_gu, gb_dn)
    return (y_out, d_tok, g_gu, gb_gu, g_dn, gb_dn, g_r.T, g_br.reshape(E), g_n.reshape(D))


def solution(mesh):
    tok = P(("dp", "ep"), None)
    w3 = P("ep", None, None)
    w2 = P("ep", None)
    in_specs = (tok, tok, tok, P(), P(), P(), w3, w2, w3, w2)
    out_specs = (tok, tok, w3, w2, w3, w2, P(), P(), P())
    return jax.shard_map(block_body, mesh=mesh, in_specs=in_specs, out_specs=out_specs, check_vma=False)
```

```python
import functools

import jax
import jax.numpy as jnp
from jax import lax
from jax.experimental import pallas as pl
from jax.experimental.pallas import tpu as pltpu
from jax.sharding import PartitionSpec as P

SWIGLU_LIMIT = 7.0
SIG_ALPHA = 1.702
NORM_EPS = 1e-5
F32 = jnp.float32
BF16 = jnp.bfloat16
MESH = pl.DeviceIdType.MESH
NT = (((1,), (1,)), ((), ()))
D = 1024
F = 512
E = 32
EL = 4
T = 128
NC = 2
TT = NC * T
FF = NC * F
LN = 128
N = 16 * T
ROWS = 16
COLS = 128
MERGE_IT = 7
FETCH_D = 2


def mid_of(m):
    return (m + 1) // 2 % 2


def col_sum(v):
    return jnp.sum(v, axis=0, keepdims=True)


def row_mean(v):
    return jnp.mean(v, axis=-1, keepdims=True)


def slot_of(m, kk):
    mid = mid_of(m)
    return mid * (1 + m + 4 * kk) + (1 - mid) * (m // 3 * 4 + kk)


def place():
    d = lax.axis_index("dp")
    e = lax.axis_index("ep")
    return d, e, e % 2, (e // 2) % 2, e // 4


def block_kernel(x_ref, idx_ref, dout_ref, nw_ref, wr_ref, br_ref, wgu_hbm, bgu_ref, wdn_hbm, bdn_ref,
                 y_out, dt_out, gbgu_ref, gbdn_ref, gr_out, gn_out, ht_hbm, a_hbm, c_hbm, v_hbm,
                 hd, pt, pb, wgu, wdn, gu, da, a_st, c_st, v_st, dyf, qs, bg, bd, py, pd, rdy, rdd,
                 rxy, rxd, ryy, ryd, riy, rid, qt, qbuf, dlog_s, gdl, ggn, ht, accg, accd,
                 ag_s, ag_r, pt_s, pt_r, d2d_s, d2d_r, rs_s, rs_r, q_s, q_r, dl_s, dl_r, gn_s, gn_r, w_sem, st_sem, h_sem):
    d, e, k, cx, cy = place()

    def ep_of(m, kk):
        return (((cy + m // 2) % 2) * 2 + (cx + m % 2) % 2) * 2 + kk

    def dev(r):
        return ((d + r // 8) % 2, ep_of((r // 2) % 4, (k + r % 2) % 2))

    sib = (d, e + 1 - 2 * k)
    zp = (1 - d, e)
    me = d * 8 + e

    for j in range(EL):
        pltpu.make_async_copy(wgu_hbm.at[j], wgu.at[j], w_sem.at[0, j]).start()
        pltpu.make_async_copy(wdn_hbm.at[j], wdn.at[j], w_sem.at[1, j]).start()

    barrier = pltpu.get_barrier_semaphore()

    @pl.loop(1, 16)
    def _(r):
        pl.semaphore_signal(barrier, inc=1, device_id=dev(r), device_id_type=MESH)

    nw = nw_ref[:].astype(F32).reshape(1, D)
    x = x_ref[:].astype(F32)
    inv = lax.rsqrt(row_mean(x * x) + NORM_EPS)
    h = (x * inv * nw).astype(BF16)
    hd[k, :, :D] = h
    hd[k, :, D:] = dout_ref[:]
    logits = lax.dot_general(h, wr_ref[:], NT, preferred_element_type=F32) + br_ref[:].reshape(1, E)
    idx = idx_ref[:].T
    lane = lax.broadcasted_iota(jnp.int32, (T, E), 1)
    hit = idx[:, 0:1] == lane
    for i in range(1, 8):
        hit = hit | (idx[:, i:i + 1] == lane)
    top = jnp.max(jnp.where(hit, logits, -jnp.inf), axis=-1, keepdims=True)
    ex = jnp.where(hit, jnp.exp(logits - top), 0.0)
    pt[k] = (ex / jnp.sum(ex, axis=-1, keepdims=True)).T

    pl.semaphore_wait(barrier, 15)

    def ag_copies(i, src, dst, to):
        return (pltpu.make_async_remote_copy(hd.at[src], hd.at[dst], ag_s.at[i], ag_r.at[i], device_id=to, device_id_type=MESH),
                pltpu.make_async_remote_copy(pt.at[src], pt.at[dst], pt_s.at[i], pt_r.at[i], device_id=to, device_id_type=MESH))

    def ag_send(i, src, dst, to):
        for cp in ag_copies(i, src, dst, to):
            cp.start()

    def ag_wait(i):
        for cp in ag_copies(i, 0, 0, sib):
            cp.wait_recv()

    def near(m):
        ag_send(m - 1, k, slot_of(m, k), (d, ep_of(m, k)))

    def fetch(m):
        ag_wait(m - 1)
        sl = slot_of(m, k)
        ag_send(7 + m, sl, sl, sib)
        ag_send(3 + m, sl, sl + 8, zp)

    def fetch_z(m):
        ag_wait(3 + m)
        sl = slot_of(m, k) + 8
        ag_send(11 + m, sl, sl, sib)

    ag_send(7, k, k, sib)

    @pl.when(k == 0)
    def _():
        near(1)
        near(2)

    ag_send(3, k, k + 8, zp)

    for j in range(EL):
        bg[j] = bgu_ref[j:j + 1, :]
        bd[j] = bdn_ref[j:j + 1, :]
    accg[:] = jnp.zeros_like(accg)
    accd[:] = jnp.zeros_like(accd)

    def mine(m):
        mid = mid_of(m)
        return mid * (1 + 2 * k) + (1 - mid) * (m // 3 * 2), mid * (m - 1) + (1 - mid) * k

    def theirs(m):
        mid = mid_of(m)
        return mid * (3 - 2 * k) + (1 - mid) * (m // 3 * 2), mid * (m - 1) + (1 - mid) * (1 - k)

    def d2d(m, hi):
        s, half = theirs(m)
        src, dst = (pd, rdd) if hi else (py, rdy)
        i = 2 * m + hi
        return pltpu.make_async_remote_copy(src.at[s, half], dst.at[m], d2d_s.at[i], d2d_r.at[i], device_id=sib, device_id_type=MESH)

    def pair_sum(m, hi):
        d2d(m, hi).wait_recv()
        s, half = mine(m)
        buf, src = (pd, rdd) if hi else (py, rdy)
        buf[s, half] += src[m]

    def rs_copy(i, hi):
        m, first, dst, to = ((1, True, (rxy, rxd), 1), (3, True, (riy, rid), 1), (1, False, (rxy, rxd), 1),
                             (2, False, (ryy, ryd), 2), (3, False, (riy, rid), 2), (2, True, (ryy, ryd), 2))[i]
        s, half = mine(m)
        cols = pl.ds(0, F) if first else pl.ds(F, F)
        n = 6 * hi + i
        return pltpu.make_async_remote_copy((py, pd)[hi].at[s, half, :, cols], dst[hi].at[:, cols], rs_s.at[n], rs_r.at[n],
                                            device_id=(d, ep_of(to, k)), device_id_type=MESH)

    def rs_start(i, n):
        for hi in (1, 0):
            rs_copy(i, hi).start()
            rs_copy(n, hi).start()

    def pair_sums(m):
        pair_sum(m, 1)
        pair_sum(m, 0)

    def relay(hi):
        buf, src = ((py, riy), (pd, rid))[hi]
        rs_copy(1, hi).wait_recv()
        s2, half2 = mine(2)
        buf[s2, half2, :, :F] += src[:, :F]
        rs_copy(4, hi).wait_recv()
        s1, half1 = mine(1)
        buf[s1, half1, :, F:] += src[:, F:]

    def q_copy(m, kk):
        i = m * 2 + (kk + k) % 2
        return pltpu.make_async_remote_copy(qt.at[slot_of(m, kk)], qbuf.at[e], q_s.at[i], q_r.at[i],
                                            device_id=(d, ep_of(m, kk)), device_id_type=MESH)

    def dl_copy(r):
        return pltpu.make_async_remote_copy(gdl.at[me], gdl.at[me], dl_s.at[r], dl_r.at[r], device_id=dev(r), device_id_type=MESH)

    def gn_copy(r):
        return pltpu.make_async_remote_copy(ggn.at[me], ggn.at[me], gn_s.at[r], gn_r.at[r], device_id=dev(r), device_id_type=MESH)

    def st_copies(par, j, slot):
        rows = pl.ds(slot * T, TT)
        return (pltpu.make_async_copy(a_st.at[par], a_hbm.at[j, rows], st_sem.at[0, par]),
                pltpu.make_async_copy(c_st.at[par], c_hbm.at[j, rows], st_sem.at[1, par]),
                pltpu.make_async_copy(v_st.at[par], v_hbm.at[j, rows], st_sem.at[2, par]))

    def ht_copy(i):
        cols = pl.ds(i * EL * T, EL * T)
        return pltpu.make_async_copy(ht.at[:, cols], ht_hbm.at[:, cols], h_sem.at[i])

    def stage_probs(slot):
        sub = lax.broadcasted_iota(jnp.int32, (E, T), 0)
        for cc in range(NC):
            dyf[cc * T:(cc + 1) * T, :] = hd[slot + cc, :, D:].astype(F32)
            rows = pt[slot + cc]
            for j in range(EL):
                row = col_sum(jnp.where(sub == 4 * e + j, rows, 0.0))
                pb[j, cc * T:(cc + 1) * T, :] = jnp.broadcast_to(row, (T, T)).T

    def expert(s, j, slot, own):
        par = j % 2
        hx = hd[pl.ds(slot, 2), :, :D].reshape(TT, D)
        gu[:] = jnp.dot(hx, wgu[j], preferred_element_type=F32)
        for c in range(0, D, LN):
            acc = jnp.zeros((8, LN), F32)
            for r in range(0, TT, ROWS):
                v = pb[j, r:r + ROWS, :] * dyf[r:r + ROWS, c:c + 128]
                v_st[par, r:r + ROWS, c:c + 128] = v.astype(BF16)
                acc = acc + jnp.sum(v.reshape(ROWS // 8, 8, LN), axis=0)
            accd[j, :, c:c + 128] += acc
        da[:] = lax.dot_general(v_st[par], wdn[j], NT, preferred_element_type=F32)
        for c in range(0, F, COLS):
            accl = jnp.zeros((8, COLS), F32)
            accu = jnp.zeros((8, COLS), F32)
            for r in range(0, TT, ROWS):
                gpre = gu[r:r + ROWS, c:c + COLS] + bg[j, :, c:c + COLS]
                upre = gu[r:r + ROWS, F + c:F + c + COLS] + bg[j, :, F + c:F + c + COLS]
                gc = jnp.minimum(gpre, SWIGLU_LIMIT)
                sg = jax.nn.sigmoid(SIG_ALPHA * gc)
                gs = gc * sg
                u1 = jnp.clip(upre, -SWIGLU_LIMIT, SWIGLU_LIMIT) + 1.0
                a_st[par, r:r + ROWS, c:c + COLS] = (gs * u1).astype(BF16)
                gu[r:r + ROWS, c:c + COLS] = jnp.where(gpre < SWIGLU_LIMIT, u1 * (sg + SIG_ALPHA * gs * (1.0 - sg)), 0.0)
                gu[r:r + ROWS, F + c:F + c + COLS] = jnp.where(jnp.abs(upre) < SWIGLU_LIMIT, gs, 0.0)
            for r in range(0, TT, ROWS):
                dact = da[r:r + ROWS, c:c + COLS]
                dg = dact * gu[r:r + ROWS, c:c + COLS]
                du = dact * gu[r:r + ROWS, F + c:F + c + COLS]
                c_st[par, r:r + ROWS, c:c + COLS] = dg.astype(BF16)
                c_st[par, r:r + ROWS, F + c:F + c + COLS] = du.astype(BF16)
                accl = accl + jnp.sum(dg.reshape(ROWS // 8, 8, COLS), axis=0)
                accu = accu + jnp.sum(du.reshape(ROWS // 8, 8, COLS), axis=0)
            accg[j, :, c:c + COLS] += accl
            accg[j, :, F + c:F + c + COLS] += accu
        if own:
            for c in range(0, D, 256):
                yv = jnp.dot(a_st[par], wdn[j, :, c:c + 256], preferred_element_type=F32)
                for r in range(0, TT, ROWS):
                    p = pb[j, r:r + ROWS, :]
                    cc, rt = r // T, r % T
                    q = None
                    for b in range(0, 256, LN):
                        y1 = yv[r:r + ROWS, b:b + LN] + bd[j, :, c + b:c + b + LN]
                        py[s, cc, rt:rt + ROWS, c + b:c + b + LN] += p * y1
                        t = dyf[r:r + ROWS, c + b:c + b + LN] * y1
                        q = t if q is None else q + t
                    if c == 0:
                        qs[r:r + ROWS, :] = q
                    else:
                        qs[r:r + ROWS, :] += q
            for c in range(0, D, 256):
                dv = lax.dot_general(c_st[par], wgu[j, c:c + 256, :], NT, preferred_element_type=F32)
                pd[s, :, :, c:c + 256] += dv.reshape(2, T, 256)
            sub = lax.broadcasted_iota(jnp.int32, (8, T), 0)
            for cc in range(NC):
                row = col_sum(qs[cc * T:(cc + 1) * T, :].T)
                qt[slot + cc] = jnp.where(sub == j, row, qt[slot + cc])

    def drain(par):
        for cp in st_copies(par, 0, 0):
            cp.wait()

    @pl.loop(0, 4)
    def _(s):
        slot = 2 * s

        @pl.when(s == 0)
        def _():
            ag_wait(7)

        @pl.when(s == 2)
        def _():
            ag_wait(10)

        @pl.when(s + 2 * k == 3)
        def _():
            ag_wait(8)
            ag_wait(9)

        stage_probs(slot)
        py[s] = jnp.zeros((NC, T, D), F32)
        pd[s] = jnp.zeros((NC, T, D), F32)
        qt[slot] = jnp.zeros((8, T), F32)
        qt[slot + 1] = jnp.zeros((8, T), F32)

        @pl.loop(0, EL)
        def _(j):
            it = s * EL + j

            @pl.when(s == 0)
            def _():
                pltpu.make_async_copy(wgu_hbm.at[j], wgu.at[j], w_sem.at[0, j]).wait()
                pltpu.make_async_copy(wdn_hbm.at[j], wdn.at[j], w_sem.at[1, j]).wait()

            @pl.when(it >= 2)
            def _():
                drain(j % 2)

            expert(s, j, slot, True)

            @pl.when(it == 6)
            def _():
                pair_sum(0, 0)
                pair_sum(0, 1)

            @pl.when(it == 12)
            def _():
                pair_sum(3, 1)

            for cp in st_copies(j % 2, j, slot):
                cp.start()

            @pl.when((it == 1) & (k == 1))
            def _():
                near(1)
                near(2)

            @pl.when((it == 2) & (k == 0))
            def _():
                fetch(1)
                ag_send(2, slot_of(1, k), slot_of(3, k), (d, ep_of(2, k)))
                fetch(2)

            @pl.when((it == 5) & (k == 1))
            def _():
                fetch(2)
                ag_send(2, slot_of(2, k), slot_of(3, k), (d, ep_of(1, k)))
                fetch(1)

            @pl.when(it == 5)
            def _():
                fetch_z(0)

            @pl.when(it == 12 + 3 * k)
            def _():
                fetch_z(1)
                fetch_z(2)

            @pl.when(it == 12)
            def _():
                rs_copy(1, 1).start()
                rs_copy(4, 1).start()
                pair_sum(3, 0)

            @pl.when(it == 3)
            def _():
                d2d(0, 0).start()
                d2d(0, 1).start()

            @pl.when(it == 15 - 8 * k)
            def _():
                d2d(1, 1).start()
                d2d(2, 1).start()
                d2d(1, 0).start()
                d2d(2, 0).start()

            @pl.when(it == 11)
            def _():
                d2d(3, 1).start()
                d2d(3, 0).start()

            @pl.when(it == 12)
            def _():
                rs_copy(1, 0).start()
                rs_copy(4, 0).start()

        @pl.when(s == 1)
        def _():
            ag_wait(11)
            stage_probs(8)

            @pl.loop(0, EL)
            def _(j):
                drain(j % 2)
                expert(0, j, 8, False)

                @pl.when((j == 2) & (k == 0))
                def _():
                    pair_sums(1)
                    pair_sums(2)

                for cp in st_copies(j % 2, j, 8):
                    cp.start()

                @pl.when((j == 2) & (k == 0))
                def _():
                    rs_start(0, 3)

                @pl.when(j == FETCH_D)
                def _():
                    fetch(3)

        for half in range(NC):
            mid = s % 2
            m = mid * (1 + half) + (1 - mid) * (s // 2) * 3
            kk = mid * (s // 2) + (1 - mid) * half

            @pl.when((m > 0) | (kk != k))
            def _():
                q_copy(m, kk).start()

    @pl.loop(1, 4)
    def _(s):
        slot = 8 + 2 * s

        @pl.when(s == 2)
        def _():
            ag_wait(14)

        @pl.when(s + 2 * k == 3)
        def _():
            ag_wait(12)
            ag_wait(13)

        stage_probs(slot)

        @pl.loop(0, EL)
        def _(j):
            it = s * EL + j
            drain(j % 2)
            expert(s, j, slot, False)

            @pl.when((it == 6) & (k == 1))
            def _():
                pair_sums(1)
                pair_sums(2)

            @pl.when(it == MERGE_IT)
            def _():
                relay(1)

            @pl.when(it == MERGE_IT + 2)
            def _():
                relay(0)

            for cp in st_copies(j % 2, j, slot):
                cp.start()

            @pl.when((it == 6) & (k == 1))
            def _():
                rs_start(0, 3)

            @pl.when(it == MERGE_IT)
            def _():
                rs_copy(5, 1).start()
                rs_copy(2, 1).start()

            @pl.when(it == MERGE_IT + 2)
            def _():
                rs_copy(5, 0).start()
                rs_copy(2, 0).start()

            @pl.when(it == 6)
            def _():
                fetch_z(3)

            @pl.when(it == 8)
            def _():
                qbuf[e] = qt[k]
                for i in range(1, 8):
                    pltpu.make_async_remote_copy(qt.at[0], qbuf.at[e], q_s.at[i], q_r.at[i], device_id=sib, device_id_type=MESH).wait_recv()
                q = jnp.concatenate([qbuf[i, :EL, :] for i in range(8)], axis=0)
                prob = pt[k]
                dlog = prob * (q - col_sum(prob * q))
                dlog_s[:] = dlog
                gdl[me] = dlog.astype(BF16)

            @pl.when(it == 9)
            def _():
                @pl.loop(1, 16)
                def _(r):
                    dl_copy(r).start()

    for par in range(NC):
        drain(par)
    for j in range(EL):
        gbgu_ref[j:j + 1, :] = col_sum(accg[j])
        gbdn_ref[j:j + 1, :] = col_sum(accd[j])

    x = x_ref[:].astype(F32)
    inv = lax.rsqrt(row_mean(x * x) + NORM_EPS)
    normed = x * inv
    dlog = dlog_s[:].T
    dhr = jnp.dot(dlog.astype(BF16), wr_ref[:], preferred_element_type=F32)
    for i in (0, 3, 5, 2):
        rs_copy(i, 1).wait_recv()
    d_h = pd[0, k] + rxd[:] + ryd[:] + dhr
    gn = col_sum(d_h * normed)
    for i in range(8):
        ggn[me, i:i + 1, :] = gn[:, i * 128:(i + 1) * 128]
    ggn[me, 8:16, :] = jnp.zeros((8, LN), F32)
    ggn[me, 8:9, :E] = col_sum(dlog)

    @pl.loop(1, 16)
    def _(r):
        gn_copy(r).start()

    dn = d_h * nw_ref[:].astype(F32).reshape(1, D)
    dt_out[:] = (dout_ref[:].astype(F32) + inv * (dn - normed * row_mean(dn * normed))).astype(BF16)

    for i in range(4):
        for g in range(EL * i, EL * i + EL):
            ht[:, g * T:(g + 1) * T] = hd[g, :, :D].T
        ht_copy(i).start()

    @pl.loop(1, 16)
    def _(r):
        dl_copy(r).wait()

    gr = jnp.zeros((E, D), F32)
    for g in range(16):
        dd, yy, xx, kk = g // 8, g // 4 % 2, g // 2 % 2, g % 2
        slot = 8 * ((dd + d) % 2) + slot_of((xx + cx) % 2 + 2 * ((yy + cy) % 2), kk)
        gr = gr + jnp.dot(gdl[g], hd[slot, :, :D], preferred_element_type=F32)
    gr_out[:] = gr
    for i in (0, 3, 5, 2):
        rs_copy(i, 0).wait_recv()
    y_out[:] = (x_ref[:].astype(F32) + (py[0, k] + rxy[:] + ryy[:])).astype(BF16)

    for i in range(15):
        for cp in ag_copies(i, 0, 0, sib):
            cp.wait_send()
    for m in range(4):
        d2d(m, 0).wait_send()
        d2d(m, 1).wait_send()
    for i in range(6):
        rs_copy(i, 0).wait_send()
        rs_copy(i, 1).wait_send()
    for i in range(1, 8):
        pltpu.make_async_remote_copy(qt.at[0], qbuf.at[e], q_s.at[i], q_r.at[i], device_id=sib, device_id_type=MESH).wait_send()

    @pl.loop(1, 16)
    def _(r):
        gn_copy(r).wait()

    gn_out[:] = ggn[:]
    for i in range(4):
        ht_copy(i).wait()


def grads_kernel(h_ref, a_ref, c_ref, v_ref, gri_ref, g_ref, yi_ref, ti_ref, bgi_ref, bdi_ref,
                 ggu_ref, gdn_ref, gr_ref, gbr_ref, gn_ref, yo_ref, to_ref, bgo_ref, bdo_ref, at):
    @pl.when((pl.program_id(0) == 0) & (pl.program_id(1) == 0))
    def _():
        gn = jnp.zeros((16, LN), F32)
        for g in range(16):
            gn = gn + g_ref[g]
        gr_ref[:] = gri_ref[:]
        gbr_ref[:] = gn[8:9, :E]
        gn_ref[:] = gn[:8]
        yo_ref[:] = yi_ref[:]
        to_ref[:] = ti_ref[:]
        bgo_ref[:] = bgi_ref[:]
        bdo_ref[:] = bdi_ref[:]

    for g in range(16):
        at[:, g * T:(g + 1) * T] = a_ref[0, g * T:(g + 1) * T, :].T
    ggu_ref[0] = jnp.dot(h_ref[:], c_ref[0], preferred_element_type=F32)
    gdn_ref[0] = jnp.dot(at[:], v_ref[0], preferred_element_type=F32)


def block_body(x_tokens, expert_idx, d_out, norm_w, w_router, b_router, w_gate_up, b_gate_up, w_down, b_down):
    vm = pl.BlockSpec(memory_space=pltpu.VMEM)
    hb = pl.BlockSpec(memory_space=pl.ANY)
    s = jax.ShapeDtypeStruct
    dma = pltpu.SemaphoreType.DMA
    out = pl.pallas_call(
        block_kernel,
        out_shape=(s((T, D), BF16), s((T, D), BF16), s((EL, D), F32), s((EL, D), F32), s((E, D), F32), s((16, 16, LN), F32),
                   s((D, N), BF16), s((EL, N, F), BF16), s((EL, N, FF), BF16), s((EL, N, D), BF16)),
        in_specs=[vm, vm, vm, vm, vm, vm, hb, vm, hb, vm],
        out_specs=(vm, vm, vm, vm, vm, vm, hb, hb, hb, hb),
        scratch_shapes=[
            pltpu.VMEM((16, T, 2 * D), BF16),
            pltpu.VMEM((16, E, T), F32),
            pltpu.VMEM((EL, TT, LN), F32),
            pltpu.VMEM((EL, D, FF), BF16),
            pltpu.VMEM((EL, F, D), BF16),
            pltpu.VMEM((TT, FF), F32),
            pltpu.VMEM((TT, F), F32),
            pltpu.VMEM((2, TT, F), BF16),
            pltpu.VMEM((2, TT, FF), BF16),
            pltpu.VMEM((2, TT, D), BF16),
            pltpu.VMEM((TT, D), F32),
            pltpu.VMEM((TT, LN), F32),
            pltpu.VMEM((EL, 1, FF), F32),
            pltpu.VMEM((EL, 1, D), F32),
            pltpu.VMEM((4, 2, T, D), F32),
            pltpu.VMEM((4, 2, T, D), F32),
            pltpu.VMEM((4, T, D), F32),
            pltpu.VMEM((4, T, D), F32),
        ] + [pltpu.VMEM((T, D), F32)] * 6 + [
            pltpu.VMEM((8, 8, T), F32),
            pltpu.VMEM((8, 8, T), F32),
            pltpu.VMEM((E, T), F32),
            pltpu.VMEM((16, E, T), BF16),
            pltpu.VMEM((16, 16, LN), F32),
            pltpu.VMEM((D, N), BF16),
            pltpu.VMEM((EL, 8, FF), F32),
            pltpu.VMEM((EL, 8, D), F32),
        ] + [dma((15,))] * 4 + [dma((8,))] * 2 + [dma((12,))] * 2 + [dma((8,))] * 2 + [dma((16,))] * 4 + [
            dma((2, EL)), dma((3, 2)), dma((4,)),
        ],
        compiler_params=pltpu.CompilerParams(collective_id=0, has_side_effects=True, vmem_limit_bytes=62 * 1024 * 1024),
        name="moe_block",
    )(x_tokens, expert_idx.T, d_out, norm_w, w_router.T, b_router, w_gate_up, b_gate_up, w_down, b_down)
    y_out, d_tok, gb_gu, gb_dn, g_r, gn_all, h_all, a_all, c_all, v_all = out
    half = D // 2

    def full(shape):
        return pl.BlockSpec(shape, lambda j, t: (0,) * len(shape))

    g_gu, g_dn, g_r, g_br, g_n, y_out, d_tok, gb_gu, gb_dn = pl.pallas_call(
        grads_kernel,
        grid=(EL, 2),
        out_shape=(s((EL, D, FF), F32), s((EL, F, D), F32), s((E, D), F32), s((1, E), F32), s((8, LN), F32),
                   s((T, D), BF16), s((T, D), BF16), s((EL, D), F32), s((EL, D), F32)),
        in_specs=[
            full((D, N)),
            pl.BlockSpec((1, N, F), lambda j, t: (j, 0, 0)),
            pl.BlockSpec((1, N, half), lambda j, t: (j, 0, t)),
            pl.BlockSpec((1, N, half), lambda j, t: (j, 0, t)),
            full((E, D)), full((16, 16, LN)), full((T, D)), full((T, D)), full((EL, D)), full((EL, D)),
        ],
        out_specs=(
            pl.BlockSpec((1, D, half), lambda j, t: (j, 0, t)),
            pl.BlockSpec((1, F, half), lambda j, t: (j, 0, t)),
            full((E, D)), full((1, E)), full((8, LN)), full((T, D)), full((T, D)), full((EL, D)), full((EL, D)),
        ),
        scratch_shapes=[pltpu.VMEM((F, N), BF16)],
        compiler_params=pltpu.CompilerParams(dimension_semantics=("arbitrary", "arbitrary"), vmem_limit_bytes=60 * 1024 * 1024),
        name="weight_grads",
    )(h_all, a_all, c_all, v_all, g_r, gn_all, y_out, d_tok, gb_gu, gb_dn)
    return (y_out, d_tok, g_gu, gb_gu, g_dn, gb_dn, g_r.T, g_br.reshape(E), g_n.reshape(D))


def solution(mesh):
    tok = P(("dp", "ep"), None)
    w3 = P("ep", None, None)
    w2 = P("ep", None)
    in_specs = (tok, tok, tok, P(), P(), P(), w3, w2, w3, w2)
    out_specs = (tok, tok, w3, w2, w3, w2, P(), P(), P())
    return jax.shard_map(block_body, mesh=mesh, in_specs=in_specs, out_specs=out_specs, check_vma=False)
```
